32 devices in a mesh: gx: 4 (over z), gy: 2 (over y), gz: 4 (over x, core).
Axes of the slice: x: 2, y: 2, z: 4, core: 2. Of those that a mesh axis runs over, the one named last changes fastest.
Arguments:
- cell_counts: int32 [16, 4, 16], P('gx', 'gy', 'gz'), may hold values from 64 to 128
- grid_offset: int32 [16, 4, 16, 3, 128], P('gx', 'gy', 'gz'), may hold values from 0 to 14
- fraction: float32 [16, 4, 16, 3, 128], P('gx', 'gy', 'gz'), may hold values from 0 to 1
- species: int32 [16, 4, 16, 128], P('gx', 'gy', 'gz'), may hold values from 0 to 1
- species_density: float32 [2], replicated, may hold values from 0.01 to 0.03
- species_pair: float32 [2], replicated, may hold values from 0.05 to 0.2
- species_embed: float32 [2], replicated, may hold values from 0.5 to 2
- species_charge: float32 [2], replicated, may hold values from -3 to 3
Outputs:
- forces: float32 [16, 4, 16, 3, 128], P('gx', 'gy', 'gz')
- density: float32 [16, 4, 16, 128], P('gx', 'gy', 'gz')
The draws below stay inside these ranges and needn't reach their ends.
Inputs may be any that keep to these rules, and one draw needn't show every extreme that they name: `cell_counts`: slots below the count hold atoms; the others are padding. `grid_offset`: an atom's stencil points lie in its own cell.
All inputs are finite; a program needn't handle non-finite values.
Results may differ from the reference program's by a relative error of at most 0.0003.
Values sent between devices are 32-bit elements; how exact they have to be, the bound alone decides.
No kernel may reach another device: no remote copies, remote signals or barrier semaphores. Data moves between devices by JAX's collectives and lax.ppermute only.
A program may use at most 128 MiB of HBM per device.

```python
import math
import jax
import jax.numpy as jnp
from jax import lax

SLOTS = 128
NSPEC = 2
PPC = 16
NX = 16
NY = 4
NZ = 16


def plant(values, key, smallest, top_value):
    longest = values.shape.index(max(values.shape))
    spots = []
    for shift in (0, 1):
        where = [jax.random.randint(jax.random.fold_in(key, axis), (), 0, length) for axis, length in enumerate(values.shape)]
        where[longest] = (where[longest] + shift) % values.shape[longest]
        spots.append(tuple(where))
    return values.at[spots[0]].set(smallest).at[spots[1]].set(top_value)


def block_levels(stream_key, dims, shards, low, largest):
    def one(axis_at, blocks):
        heights = jax.random.uniform(jax.random.fold_in(jax.random.fold_in(stream_key, 6), axis_at), (blocks,), jnp.float32, low / len(shards), largest / len(shards))
        return jnp.repeat(jnp.exp(heights), dims[axis_at] // blocks).reshape((-1,) + (1,) * (len(dims) - axis_at - 1))

    factor_of = one(*shards[0])
    for cut in shards[1:]:
        factor_of = factor_of * one(*cut)
    return factor_of


def noise(stream_key, shape, scale, limit, kind=jnp.bfloat16):
    return jnp.clip(scale * jax.random.normal(stream_key, shape, jnp.float32), -limit, limit).astype(kind)


def setup_inputs(seed: int = 0) -> dict:
    arg_keys = jax.random.split(jax.random.key(seed), 9)
    return {
        "cell_counts": plant(jax.random.randint(arg_keys[0], (NX, NY, NZ), SLOTS // 2, SLOTS + 1), jax.random.fold_in(arg_keys[0], 1), SLOTS // 2, SLOTS).astype(jnp.int32),
        "grid_offset": plant(jax.random.randint(arg_keys[1], (NX, NY, NZ, 3, SLOTS), 0, PPC - 1), jax.random.fold_in(arg_keys[1], 1), 0, (PPC - 1) - 1).astype(jnp.int32),
        "fraction": jnp.clip(1.0 * jax.random.uniform(arg_keys[2], (NX, NY, NZ, 3, SLOTS), jnp.float32) ** block_levels(arg_keys[2], (NX, NY, NZ, 3, SLOTS), ((0, 4), (1, 2), (2, 4)), -0.2, 0.2), 0.0, 1.0),
        "species": plant(jax.random.randint(arg_keys[3], (NX, NY, NZ, SLOTS), 0, NSPEC), jax.random.fold_in(arg_keys[3], 1), 0, NSPEC - 1).astype(jnp.int32),
        "species_density": jnp.clip(jnp.exp(jax.random.uniform(arg_keys[4], (NSPEC,), jnp.float32, math.log(0.01), math.log(0.03))), 0.01, 0.03),
        "species_pair": jnp.clip(jnp.exp(jax.random.uniform(arg_keys[5], (NSPEC,), jnp.float32, math.log(0.05), math.log(0.2))), 0.05, 0.2),
        "species_embed": jnp.clip(jnp.exp(jax.random.uniform(arg_keys[6], (NSPEC,), jnp.float32, math.log(0.5), math.log(2.0))), 0.5, 2.0),
        "species_charge": noise(arg_keys[7], (NSPEC,), 1.0, 3.0, jnp.float32),
    }


EWALD_SPLIT = 0.7
COUPLING = 8.0
HIGHEST_PRECISION = lax.Precision.HIGHEST
neighbour_shifts = [(shift_x, shift_y, shift_z) for shift_x in (-1, 0, 1) for shift_y in (-1, 0, 1) for shift_z in (-1, 0, 1)]

def species_value(species, lookup_table):
    result = jnp.zeros(species.shape, jnp.float32)
    for kind_index in range(NSPEC):
        result = result + jnp.where(species == kind_index, lookup_table[kind_index], 0.0)
    return result

def stencil(offsets, fractions):
    points = lax.broadcasted_iota(jnp.int32, offsets.shape + (PPC,), offsets.ndim)
    lower_point = (points == offsets[..., None]).astype(jnp.float32)
    upper_point = (points == offsets[..., None] + 1).astype(jnp.float32)
    weights = lower_point * (1.0 - fractions[..., None]) + upper_point * fractions[..., None]
    return (weights, upper_point - lower_point)

def spread_cells(charges, weights_x, weights_y, weights_z):
    batch_size, slot_count = charges.shape
    pair_plane = (weights_y[:, :, :, None] * weights_z[:, :, None, :]).reshape(batch_size, slot_count, PPC * PPC)
    return jnp.einsum('bax,bay->bxy', weights_x * charges[:, :, None], pair_plane, precision=HIGHEST_PRECISION)

def outer_plane(first_weights, second_weights):
    batch_size, slot_count, width_count = first_weights.shape
    return (first_weights[:, :, :, None] * second_weights[:, :, None, :]).reshape(batch_size, slot_count, width_count * width_count)

def sample_cells(blocks, charges, weights_x, weights_y, weights_z, slope_x, slope_y, slope_z):
    plain_x = jnp.einsum('bax,bxy->bay', weights_x, blocks, precision=HIGHEST_PRECISION)
    tilted_x = jnp.einsum('bax,bxy->bay', slope_x, blocks, precision=HIGHEST_PRECISION)
    force_x = -charges * lax.optimization_barrier(jnp.sum(tilted_x * outer_plane(weights_y, weights_z), axis=2))
    force_y = -charges * lax.optimization_barrier(jnp.sum(plain_x * outer_plane(slope_y, weights_z), axis=2))
    force_z = -charges * lax.optimization_barrier(jnp.sum(plain_x * outer_plane(weights_y, slope_z), axis=2))
    return jnp.stack([force_x, force_y, force_z], axis=1)

def signed_modes(indices, total):
    return jnp.where(2 * indices >= total, indices - total, indices)

def green_factor(modes_x, modes_y, modes_z, length_x, length_y, length_z):
    wave_x = modes_x.astype(jnp.float32) * (2.0 * math.pi / length_x)
    wave_y = modes_y.astype(jnp.float32) * (2.0 * math.pi / length_y)
    wave_z = modes_z.astype(jnp.float32) * (2.0 * math.pi / length_z)
    squared = wave_x * wave_x + wave_y * wave_y + wave_z * wave_z
    anchor = (modes_x == 0) & (modes_y == 0) & (modes_z == 0)
    safe_square = jnp.where(anchor, 1.0, squared)
    return jnp.where(anchor, 0.0, 4.0 * math.pi * jnp.exp(-squared / (4.0 * EWALD_SPLIT * EWALD_SPLIT)) / safe_square)

def periodic(values):
    widths = [(1, 1), (1, 1), (1, 1)] + [(0, 0)] * (values.ndim - 3)
    return jnp.pad(values, widths, mode='wrap')

def pair_terms(positions, other_positions, shift_triple, not_self):
    shift_vector = jnp.asarray(shift_triple, jnp.float32)
    separation = shift_vector[:, None, None] + other_positions[..., :, None, :] - positions[..., :, :, None]
    squared = lax.optimization_barrier(jnp.sum(separation * separation, axis=-3))
    weight = jnp.maximum(1.0 - squared, 0.0)
    if shift_triple == (0, 0, 0):
        weight = weight * not_self
    return (separation, weight)

def window(rows, shift_triple, cells_y, cells_z):
    return rows[1 + shift_triple[0], 1 + shift_triple[1]:1 + shift_triple[1] + cells_y, 1 + shift_triple[2]:1 + shift_triple[2] + cells_z]

def reference(cell_counts, grid_offset, fraction, species, species_density, species_pair, species_embed, species_charge):
    slot_index = lax.broadcasted_iota(jnp.int32, species.shape, 3)
    alive_mask = (slot_index < cell_counts[..., None]).astype(jnp.float32)
    positions = (grid_offset.astype(jnp.float32) + 0.5 + fraction) / PPC
    density_coef = species_value(species, species_density) * alive_mask
    repulsion = species_value(species, species_pair) * alive_mask
    embedding = species_value(species, species_embed)
    charges = species_value(species, species_charge) * alive_mask
    not_self = (lax.broadcasted_iota(jnp.int32, (SLOTS, SLOTS), 0) != lax.broadcasted_iota(jnp.int32, (SLOTS, SLOTS), 1)).astype(jnp.float32)
    wide_positions = periodic(positions)
    wide_density = periodic(density_coef)
    wide_repulsion = periodic(repulsion)
    row_ids = jnp.arange(NX, dtype=jnp.int32)

    def density_row(row):
        near_pos = lax.dynamic_slice_in_dim(wide_positions, row, 3, 0)
        near_coef = lax.dynamic_slice_in_dim(wide_density, row, 3, 0)
        own = lax.dynamic_index_in_dim(positions, row, 0, keepdims=False)
        total = jnp.zeros((NY, NZ, SLOTS), jnp.float32)
        for shift_triple in neighbour_shifts:
            separation, weight = pair_terms(own, window(near_pos, shift_triple, NY, NZ), shift_triple, not_self)
            total = total + lax.optimization_barrier(jnp.sum(weight * weight * weight * window(near_coef, shift_triple, NY, NZ)[..., None, :], axis=-1))
        return total
    density = lax.map(density_row, row_ids) * alive_mask
    slope_embed = -embedding * alive_mask / (2.0 * jnp.sqrt(1.0 + density))
    wide_slope = periodic(slope_embed)

    def force_row(row):
        near_pos = lax.dynamic_slice_in_dim(wide_positions, row, 3, 0)
        near_coef = lax.dynamic_slice_in_dim(wide_density, row, 3, 0)
        near_rep = lax.dynamic_slice_in_dim(wide_repulsion, row, 3, 0)
        near_slp = lax.dynamic_slice_in_dim(wide_slope, row, 3, 0)
        own = lax.dynamic_index_in_dim(positions, row, 0, keepdims=False)
        own_rep = lax.dynamic_index_in_dim(repulsion, row, 0, keepdims=False)
        own_coef = lax.dynamic_index_in_dim(density_coef, row, 0, keepdims=False)
        own_slope = lax.dynamic_index_in_dim(slope_embed, row, 0, keepdims=False)
        total = jnp.zeros((NY, NZ, 3, SLOTS), jnp.float32)
        for shift_triple in neighbour_shifts:
            separation, weight = pair_terms(own, window(near_pos, shift_triple, NY, NZ), shift_triple, not_self)
            other_coef = window(near_coef, shift_triple, NY, NZ)[..., None, :]
            other_rep = window(near_rep, shift_triple, NY, NZ)[..., None, :]
            other_slope = window(near_slp, shift_triple, NY, NZ)[..., None, :]
            coefficient = -2.0 * own_rep[..., :, None] * other_rep * weight - 3.0 * weight * weight * (own_slope[..., :, None] * other_coef + other_slope * own_coef[..., :, None])
            total = total + 2.0 * lax.optimization_barrier(jnp.sum(coefficient[..., None, :, :] * separation, axis=-1))
        return total
    eam_force = lax.map(force_row, row_ids)
    stencils = [stencil(grid_offset[:, :, :, axis_index, :], fraction[:, :, :, axis_index, :]) for axis_index in range(3)]
    row_cells = NY * NZ

    def spread_row(row_items):
        charge_row, first_row, second_row, third_row = row_items
        return spread_cells(charge_row.reshape(row_cells, SLOTS), first_row.reshape(row_cells, SLOTS, PPC), second_row.reshape(row_cells, SLOTS, PPC), third_row.reshape(row_cells, SLOTS, PPC))
    blocks = lax.map(spread_row, (charges, stencils[0][0], stencils[1][0], stencils[2][0]))
    length_x, length_y, length_z = (NX * PPC, NY * PPC, NZ * PPC)
    charge_grid = blocks.reshape(NX, NY, NZ, PPC, PPC, PPC).transpose(0, 3, 1, 4, 2, 5).reshape(length_x, length_y, length_z)
    modes_x = signed_modes(jnp.arange(length_x, dtype=jnp.int32), length_x)[:, None, None]
    modes_y = signed_modes(jnp.arange(length_y, dtype=jnp.int32), length_y)[None, :, None]
    modes_z = signed_modes(jnp.arange(length_z, dtype=jnp.int32), length_z)[None, None, :]
    factor = green_factor(modes_x, modes_y, modes_z, length_x, length_y, length_z)
    potential = jnp.real(jnp.fft.ifftn(jnp.fft.fftn(charge_grid) * factor)).astype(jnp.float32)
    blocks_back = potential.reshape(NX, PPC, NY, PPC, NZ, PPC).transpose(0, 2, 4, 1, 3, 5).reshape(NX, row_cells, PPC, PPC * PPC)

    def sample_row(row_items):
        block_row, charge_row, first_w, second_w, third_w, first_s, second_s, third_s = row_items

        def shaped(values):
            return values.reshape(row_cells, SLOTS, PPC)
        return sample_cells(block_row, charge_row.reshape(row_cells, SLOTS), shaped(first_w), shaped(second_w), shaped(third_w), shaped(first_s), shaped(second_s), shaped(third_s))
    electric = lax.map(sample_row, (blocks_back, charges, stencils[0][0], stencils[1][0], stencils[2][0], stencils[0][1], stencils[1][1], stencils[2][1]))
    electric = electric.reshape(NX, NY, NZ, 3, SLOTS)
    forces = (eam_force + COUPLING * electric) * alive_mask[:, :, :, None, :]
    return (forces, density)
```

```python
import math

import ml_dtypes
import numpy as np

import jax
import jax.numpy as jnp
from jax import lax
from jax.experimental import pallas as pl
from jax.experimental.pallas import tpu as pltpu
from jax.sharding import PartitionSpec as P

NSPEC = 2
PPC = 16
EWALD_SPLIT = 0.7
COUPLING = 8.0
F32 = jnp.float32
BF16 = jnp.bfloat16
VMEM = pl.BlockSpec(memory_space=pltpu.VMEM)
SMEM = pl.BlockSpec(memory_space=pltpu.SMEM)
NN = (((1,), (0,)), ((), ()))
NT = (((1,), (1,)), ((), ()))
PARAMS = pltpu.CompilerParams(vmem_limit_bytes=56 * 1024 * 1024)


def split2(values):
    high = values.astype(BF16)
    return high, (values - high.astype(F32)).astype(BF16)


def split3(values):
    high = values.astype(BF16).astype(F32)
    rest = values - high
    middle = rest.astype(BF16).astype(F32)
    return high, middle, (rest - middle).astype(BF16).astype(F32)


def dot(left, right, dims):
    return lax.dot_general(left, right, dims, preferred_element_type=F32)


def dot3(left, right, dims):
    return (
        dot(left[0], right[0], dims) + dot(left[0], right[1], dims) + dot(left[1], right[0], dims)
    )


def by_kind(kind, table, column):
    result = jnp.zeros(kind.shape, F32)
    for kind_index in range(NSPEC):
        result = jnp.where(kind == float(kind_index), table[column, kind_index], result)
    return result


def real_basis(length):
    rows = np.arange(length)[:, None]
    points = np.arange(length)[None, :]
    half = length // 2
    waves = np.where(rows <= half, rows, length - rows)
    angle = 2.0 * np.pi * ((waves * points) % length) / length
    basis = np.where(rows <= half, np.cos(angle), np.sin(angle)) * math.sqrt(2.0 / length)
    basis[0] *= math.sqrt(0.5)
    basis[half] *= math.sqrt(0.5)
    return basis


def table_pair(values):
    values = values.astype(np.float32)
    high = values.astype(ml_dtypes.bfloat16)
    low = (values - high.astype(np.float32)).astype(ml_dtypes.bfloat16)
    return jnp.asarray(high), jnp.asarray(low)


def signed_modes(indices, total):
    return jnp.where(2 * indices >= total, indices - total, indices)


def green_factor(modes_x, modes_y, modes_z, length_x, length_y, length_z):
    wave_x = modes_x.astype(F32) * (2.0 * math.pi / length_x)
    wave_y = modes_y.astype(F32) * (2.0 * math.pi / length_y)
    wave_z = modes_z.astype(F32) * (2.0 * math.pi / length_z)
    squared = wave_x * wave_x + wave_y * wave_y + wave_z * wave_z
    anchor = (modes_x == 0) & (modes_y == 0) & (modes_z == 0)
    safe_square = jnp.where(anchor, 1.0, squared)
    return jnp.where(
        anchor,
        0.0,
        4.0 * math.pi * jnp.exp(-squared / (4.0 * EWALD_SPLIT * EWALD_SPLIT)) / safe_square,
    )


def chunk_transpose(tiles, chunk):
    tiles = list(tiles)
    count = len(tiles)
    width = tiles[0].shape[-1]
    lane_chunk = lax.broadcasted_iota(jnp.int32, tiles[0].shape, 1) // chunk
    bit = 1
    while bit < count:
        keep = (lane_chunk & bit) == 0
        for low in range(count):
            if low & bit:
                continue
            first, second = tiles[low], tiles[low | bit]
            tiles[low] = jnp.where(keep, first, pltpu.roll(second, bit * chunk, 1))
            tiles[low | bit] = jnp.where(keep, pltpu.roll(first, width - bit * chunk, 1), second)
        bit *= 2
    return tiles


def point_weights(offset_row, fraction_row):
    points = lax.broadcasted_iota(jnp.int32, (PPC, offset_row.shape[-1]), 0).astype(F32)
    lower = points == offset_row
    upper = points == offset_row + 1.0
    weights = jnp.where(lower, 1.0 - fraction_row, jnp.where(upper, fraction_row, 0.0))
    slopes = jnp.where(lower, -1.0, jnp.where(upper, 1.0, 0.0))
    return weights, slopes


def make_spread(parts, cells_y, cells_z, slots, lz, devices, relayout):
    columns = parts * cells_z
    modes = lz // devices
    yl = cells_y * PPC
    rows = PPC * PPC

    def kernel(atoms, table, basis_hi, basis_lo, out, plane_hi, plane_lo, line_hi, line_lo):
        line_hi[...] = jnp.zeros(line_hi.shape, BF16)
        line_lo[...] = jnp.zeros(line_lo.shape, BF16)
        basis = (basis_hi[...], basis_lo[...])
        pieces = []
        for cy in range(cells_y):
            for column in range(columns):
                cell = atoms[column // cells_z, cy, column % cells_z]
                weights = [point_weights(cell[d : d + 1], cell[3 + d : 4 + d])[0] for d in range(3)]
                along_x = weights[0] * by_kind(cell[6:7], table, 3)
                plane = jnp.concatenate(
                    [weights[1][y : y + 1] * along_x for y in range(PPC)], axis=0
                )
                lanes = pl.ds(column * slots, slots)
                points = pl.ds(column * PPC, PPC)
                plane_hi[:, lanes], plane_lo[:, lanes] = split2(plane)
                line_hi[points, lanes], line_lo[points, lanes] = split2(weights[2])
            brick = dot3(
                (plane_hi[...], plane_lo[...]), (line_hi[...], line_lo[...]), NT
            )
            pieces.append(dot3(split2(brick), basis, NT))
        if not relayout:
            for cy in range(cells_y):
                out[pl.ds(cy * rows, rows), :] = pieces[cy]
            return
        chunks = 128 // modes
        for tile in range(lz // 128):
            for group in range(yl // chunks):
                tiles = []
                for y in range(group * chunks, (group + 1) * chunks):
                    start = (y % PPC) * PPC
                    tiles.append(
                        pieces[y // PPC][start : start + PPC, tile * 128 : tile * 128 + 128]
                    )
                for chunk, value in enumerate(chunk_transpose(tiles, modes)):
                    out[tile * chunks + chunk, :, pl.ds(group * 128, 128)] = value

    if relayout:
        shape = (devices, PPC, yl * modes)
    else:
        shape = (cells_y * rows, lz)
    return pl.pallas_call(
        kernel,
        out_shape=jax.ShapeDtypeStruct(shape, F32),
        in_specs=[VMEM, SMEM, VMEM, VMEM],
        out_specs=VMEM,
        scratch_shapes=[
            pltpu.VMEM((rows, columns * slots), BF16),
            pltpu.VMEM((rows, columns * slots), BF16),
            pltpu.VMEM((lz, columns * slots), BF16),
            pltpu.VMEM((lz, columns * slots), BF16),
        ],
        compiler_params=PARAMS,
        name="spread",
    )


def make_planes(gx, gy, gz, lanes, lx, width):
    def kernel(data, x_hi, x_lo, xt_hi, xt_lo, y_hi, y_lo, green, out, grid):
        for a in range(gx):
            for b in range(gy):
                for c in range(gz):
                    grid[pl.ds((a * gz + c) * PPC, PPC), pl.ds(b * lanes, lanes)] = data[
                        (a * gy + b) * gz + c
                    ]
        along_y = (y_hi[...], y_lo[...])
        value = dot3((x_hi[...], x_lo[...]), split2(grid[...]), NN)
        value = dot3(split2(value), along_y, NT) * green[...]
        value = dot3(split2(value), along_y, NN)
        value = dot3((xt_hi[...], xt_lo[...]), split2(value), NN)
        for a in range(gx):
            for b in range(gy):
                for c in range(gz):
                    start = (a * gz + c) * PPC
                    out[(a * gy + b) * gz + c] = value[
                        start : start + PPC, b * lanes : (b + 1) * lanes
                    ]

    return pl.pallas_call(
        kernel,
        out_shape=jax.ShapeDtypeStruct((gx * gy * gz, PPC, lanes), F32),
        in_specs=[VMEM] * 8,
        out_specs=VMEM,
        scratch_shapes=[pltpu.VMEM((lx, width), F32)],
        compiler_params=PARAMS,
        name="planes",
    )


def make_sample(parts, cells_y, cells_z, slots, lz, devices, relayout):
    columns = parts * cells_z
    modes = lz // devices
    yl = cells_y * PPC
    rows = PPC * PPC

    def kernel(data, atoms, table, basis_hi, basis_lo, out, lines, line_hi, line_lo):
        if relayout:
            chunks = 128 // modes
            for tile in range(lz // 128):
                for group in range(yl // chunks):
                    tiles = [
                        data[tile * chunks + chunk, :, pl.ds(group * 128, 128)]
                        for chunk in range(chunks)
                    ]
                    for index, value in enumerate(chunk_transpose(tiles, modes)):
                        lines[
                            pl.ds((group * chunks + index) * PPC, PPC), pl.ds(tile * 128, 128)
                        ] = value
        else:
            lines[...] = data[...]
        line_hi[...] = jnp.zeros(line_hi.shape, BF16)
        line_lo[...] = jnp.zeros(line_lo.shape, BF16)
        basis = (basis_hi[...], basis_lo[...])
        for cy in range(cells_y):
            brick = split2(dot3(split2(lines[pl.ds(cy * rows, rows), :]), basis, NN))
            for column in range(columns):
                cell = atoms[column // cells_z, cy, column % cells_z]
                pairs = [point_weights(cell[d : d + 1], cell[3 + d : 4 + d]) for d in range(3)]
                (wx, sx), (wy, sy), (wz, sz) = pairs
                points = pl.ds(column * PPC, PPC)
                high, low = split2(wz)
                line_hi[column, points, pl.ds(0, slots)] = high
                line_hi[column, points, pl.ds(slots, slots)] = sz.astype(BF16)
                line_lo[column, points, :] = low
                both = dot(brick[0], line_hi[column], NN) + dot(brick[1], line_hi[column], NN)
                plain = both[:, :slots] + dot(brick[0], line_lo[column], NN)
                tilted = both[:, slots:]
                force_x = jnp.zeros((PPC, slots), F32)
                force_y = jnp.zeros((PPC, slots), F32)
                force_z = jnp.zeros((PPC, slots), F32)
                for y in range(PPC):
                    block = plain[y * PPC : (y + 1) * PPC]
                    force_x += wy[y : y + 1] * block
                    force_y += sy[y : y + 1] * block
                    force_z += wy[y : y + 1] * tilted[y * PPC : (y + 1) * PPC]
                charge = -by_kind(cell[6:7], table, 3)
                result = [
                    charge * jnp.sum(force * weight, axis=0, keepdims=True)
                    for force, weight in ((force_x, sx), (force_y, wx), (force_z, wx))
                ]
                out[column // cells_z, cy, column % cells_z] = jnp.concatenate(result, axis=0)

    return pl.pallas_call(
        kernel,
        out_shape=jax.ShapeDtypeStruct((parts, cells_y, cells_z, 3, slots), F32),
        in_specs=[VMEM, VMEM, SMEM, VMEM, VMEM],
        out_specs=VMEM,
        scratch_shapes=[
            pltpu.VMEM((cells_y * rows, lz), F32),
            pltpu.VMEM((columns, lz, 2 * slots), BF16),
            pltpu.VMEM((columns, lz, slots), BF16),
        ],
        compiler_params=PARAMS,
        name="sample",
    )


ORDER = ((0, 0), (1, 0), (0, 1), (1, 1), (2, 0), (0, 2))


def spread_pieces(values, side):
    pieces = split3(values)
    stacked = [pieces[entry[side]] for entry in ORDER]
    stacked += [jnp.zeros_like(values)] * 2
    return jnp.concatenate(stacked, axis=0)


def cell_positions(ext, x, y, sizes):
    count_x, count_y, count_z = sizes
    along_z = lax.broadcasted_iota(jnp.int32, (count_z, ext.shape[-1]), 0).astype(F32)
    pos_x = ext[x, y, :, 0, :] + (x - 0.5 * count_x)
    pos_y = ext[x, y, :, 1, :] + (y - 0.5 * count_y)
    pos_z = ext[x, y, :, 2, :] + (along_z - 0.5 * count_z)
    return (pos_x, pos_y, pos_z)


def cell_at(index, cells):
    cells_x, cells_y, cells_z = cells
    x = index // (cells_y * cells_z)
    y = (index // cells_z) % cells_y
    z = index % cells_z
    return x, y, z


def make_density(cells, slots):
    cells_x, cells_y, cells_z = cells
    sizes = (cells_x + 2, cells_y + 2, cells_z + 2)
    own = cells_x * cells_y * cells_z
    total = sizes[0] * sizes[1] * sizes[2]

    def kernel(ext, table, density, slope, feature, own_feature, right, left, sums):
        feature[...] = jnp.zeros(feature.shape, F32)
        own_feature[...] = jnp.zeros(own_feature.shape, F32)
        for x in range(sizes[0]):
            for y in range(sizes[1]):
                pos = cell_positions(ext, x, y, sizes)
                square = pos[0] * pos[0] + pos[1] * pos[1] + pos[2] * pos[2]
                scale = by_kind(ext[x, y, :, 3, :], table, 4)
                base = (x * sizes[1] + y) * sizes[2]
                here = pl.ds(base, sizes[2])
                feature[here, 0, :] = scale * (1.0 - square)
                for d in range(3):
                    feature[here, 1 + d, :] = 2.0 * scale * pos[d]
                feature[here, 4, :] = -scale
                if 1 <= x <= cells_x and 1 <= y <= cells_y:
                    there = pl.ds(((x - 1) * cells_y + y - 1) * cells_z, cells_z)
                    own_feature[there, 0, :] = jnp.ones((cells_z, slots), F32)
                    for d in range(3):
                        own_feature[there, 1 + d, :] = pos[d][1 : 1 + cells_z]
                    own_feature[there, 4, :] = square[1 : 1 + cells_z]

        def fill_right(n, carry):
            right[n] = spread_pieces(feature[n], 0).astype(BF16)
            return carry

        def fill_left(n, carry):
            left[n] = spread_pieces(own_feature[n], 1).T.astype(BF16)
            return carry

        lax.fori_loop(0, total, fill_right, 0, unroll=8)
        lax.fori_loop(0, own, fill_left, 0, unroll=4)
        same = lax.broadcasted_iota(jnp.int32, (slots, slots), 0) == lax.broadcasted_iota(
            jnp.int32, (slots, slots), 1
        )
        lane = lax.broadcasted_iota(jnp.int32, (slots, 128), 1)
        sums[...] = jnp.zeros(sums.shape, F32)
        near = [
            (dx * sizes[1] + dy) * sizes[2] + dz
            for dx in range(3)
            for dy in range(3)
            for dz in range(3)
        ]
        centre = near.pop(13)

        def one_cell(n, carry):
            x, y, z = cell_at(n, cells)
            base = (x * sizes[1] + y) * sizes[2] + z
            lhs = left[n]
            weight = jnp.maximum(dot(lhs, right[base + centre], NN), 0.0)
            weight = jnp.where(same, 0.0, weight)
            total_sum = weight * weight * weight
            for first, second in zip(near[0::2], near[1::2]):
                rhs = jnp.concatenate([right[base + first], right[base + second]], axis=1)
                weight = jnp.maximum(dot(lhs, rhs, NN), 0.0)
                cube = weight * weight * weight
                total_sum = total_sum + cube[:, :slots] + cube[:, slots:]
            column = jnp.sum(total_sum, axis=1, keepdims=True)
            sums[...] = jnp.where(lane == n, column, sums[...])
            return carry

        lax.fori_loop(0, own, one_cell, 0)
        rows = sums[...].T
        for x in range(cells_x):
            for y in range(cells_y):
                start = (x * cells_y + y) * cells_z
                kind = ext[x + 1, y + 1, :, 3, :][1 : 1 + cells_z]
                value = jnp.where(kind >= 0.0, rows[start : start + cells_z], 0.0)
                density[x, y] = value
                slope[x, y] = -by_kind(kind, table, 2) / (2.0 * jnp.sqrt(1.0 + value))

    shape = jax.ShapeDtypeStruct((cells_x, cells_y, cells_z, slots), F32)
    return pl.pallas_call(
        kernel,
        out_shape=(shape, shape),
        in_specs=[VMEM, SMEM],
        out_specs=(VMEM, VMEM),
        scratch_shapes=[
            pltpu.VMEM((total, 8, slots), F32),
            pltpu.VMEM((own, 8, slots), F32),
            pltpu.VMEM((total, 64, slots), BF16),
            pltpu.VMEM((own, slots, 64), BF16),
            pltpu.VMEM((slots, 128), F32),
        ],
        compiler_params=PARAMS,
        cost_estimate=pl.CostEstimate(
            flops=own * 27 * slots * slots * 40, bytes_accessed=total * slots * 16, transcendentals=0
        ),
        name="density",
    )


def make_force(cells, slots):
    cells_x, cells_y, cells_z = cells
    sizes = (cells_x + 2, cells_y + 2, cells_z + 2)
    own = cells_x * cells_y * cells_z
    total = sizes[0] * sizes[1] * sizes[2]
    chunk = 32

    def kernel(ext, slopes, table, out, feature, own_feature, place, right, left, both, sums):
        feature[...] = jnp.zeros(feature.shape, F32)
        own_feature[...] = jnp.zeros(own_feature.shape, F32)
        for x in range(sizes[0]):
            for y in range(sizes[1]):
                pos = cell_positions(ext, x, y, sizes)
                square = pos[0] * pos[0] + pos[1] * pos[1] + pos[2] * pos[2]
                kind = ext[x, y, :, 3, :]
                scale = by_kind(kind, table, 1)
                steep = slopes[x, y] * by_kind(kind, table, 5)
                mild = by_kind(kind, table, 6)
                here = pl.ds((x * sizes[1] + y) * sizes[2], sizes[2])
                feature[here, 0, :] = scale * (1.0 - square)
                for d in range(3):
                    feature[here, 1 + d, :] = 2.0 * scale * pos[d]
                    place[here, d, :] = pos[d]
                feature[here, 4, :] = -scale
                feature[here, 8, :] = steep
                feature[here, 9, :] = mild
                if 1 <= x <= cells_x and 1 <= y <= cells_y:
                    inner = slice(1, 1 + cells_z)
                    there = pl.ds(((x - 1) * cells_y + y - 1) * cells_z, cells_z)
                    own_feature[there, 0, :] = scale[inner]
                    for d in range(3):
                        own_feature[there, 1 + d, :] = (scale * pos[d])[inner]
                    own_feature[there, 4, :] = (scale * square)[inner]
                    own_feature[there, 8, :] = mild[inner]
                    own_feature[there, 9, :] = steep[inner]

        def fill_right(n, carry):
            values = feature[n]
            right[n, pl.ds(0, 64), :] = spread_pieces(values[0:8], 0).astype(BF16)
            right[n, pl.ds(64, 64), :] = spread_pieces(values[8:16], 0).astype(BF16)
            return carry

        def fill_left(n, carry):
            values = own_feature[n]
            left[n, :, pl.ds(0, 64)] = spread_pieces(values[0:8], 1).T.astype(BF16)
            left[n, :, pl.ds(64, 64)] = spread_pieces(values[8:16], 1).T.astype(BF16)
            return carry

        lax.fori_loop(0, total, fill_right, 0, unroll=8)
        lax.fori_loop(0, own, fill_left, 0, unroll=4)
        same = lax.broadcasted_iota(jnp.int32, (slots, slots), 0) == lax.broadcasted_iota(
            jnp.int32, (slots, slots), 1
        )
        lane = lax.broadcasted_iota(jnp.int32, (slots, 128), 1)
        sums[...] = jnp.zeros(sums.shape, F32)
        near = [
            (dx * sizes[1] + dy) * sizes[2] + dz
            for dx in range(3)
            for dy in range(3)
            for dz in range(3)
        ]
        centre = near.pop(13)
        near = [centre] + near

        def products(n, slot):
            x, y, z = cell_at(n, cells)
            base = (x * sizes[1] + y) * sizes[2] + z
            lhs = (left[n, :, pl.ds(0, 64)], left[n, :, pl.ds(64, 64)])
            for part in range(2):
                rows = pl.ds(part * 64, 64)
                value = dot(lhs[part], right[base + centre, rows, :], NN)
                if part == 0:
                    value = jnp.where(same, 0.0, value)
                both[slot, part, 0] = value
                for index in range(1, 27, 2):
                    rhs = jnp.concatenate(
                        [right[base + near[index], rows, :], right[base + near[index + 1], rows, :]],
                        axis=1,
                    )
                    value = dot(lhs[part], rhs, NN)
                    both[slot, part, index] = value[:, :slots]
                    both[slot, part, index + 1] = value[:, slots:]

        products(0, 0)

        def one_cell(n, carry):
            slot = n % 2
            x, y, z = cell_at(n, cells)
            base = (x * sizes[1] + y) * sizes[2] + z
            products(jnp.minimum(n + 1, own - 1), 1 - slot)
            for start in range(0, slots, chunk):
                rows = pl.ds(start, chunk)
                acc = [jnp.zeros((chunk, slots), F32) for _ in range(4)]
                for index in range(27):
                    weight = jnp.maximum(both[slot, 0, index, rows, :], 0.0)
                    value = (weight * both[slot, 1, index, rows, :] - 2.0) * weight
                    acc[3] = acc[3] + value
                    for d in range(3):
                        acc[d] = acc[d] + value * place[base + near[index], pl.ds(d, 1), :]
                for d in range(4):
                    column = jnp.sum(acc[d], axis=1, keepdims=True)
                    sums[d, rows, :] = jnp.where(
                        lane[start : start + chunk] == n, column, sums[d, rows, :]
                    )
            return carry

        lax.fori_loop(0, own, one_cell, 0)
        rows = [sums[d].T for d in range(4)]
        for x in range(cells_x):
            for y in range(cells_y):
                start = (x * cells_y + y) * cells_z
                stop = start + cells_z
                pos = cell_positions(ext, x + 1, y + 1, sizes)
                for d in range(3):
                    out[x, y, :, d, :] = 2.0 * (
                        rows[d][start:stop] - pos[d][1 : 1 + cells_z] * rows[3][start:stop]
                    )

    return pl.pallas_call(
        kernel,
        out_shape=jax.ShapeDtypeStruct((cells_x, cells_y, cells_z, 3, slots), F32),
        in_specs=[VMEM, VMEM, SMEM],
        out_specs=VMEM,
        scratch_shapes=[
            pltpu.VMEM((total, 16, slots), F32),
            pltpu.VMEM((own, 16, slots), F32),
            pltpu.VMEM((total, 8, slots), F32),
            pltpu.VMEM((total, 128, slots), BF16),
            pltpu.VMEM((own, slots, 128), BF16),
            pltpu.VMEM((2, 2, 27, slots, slots), F32),
            pltpu.VMEM((4, slots, 128), F32),
        ],
        compiler_params=PARAMS,
        cost_estimate=pl.CostEstimate(
            flops=own * 27 * slots * slots * 100,
            bytes_accessed=total * slots * 16,
            transcendentals=0,
        ),
        name="force",
    )


def padded(block, sides, width):
    for axis, dim in sides:
        count = lax.axis_size(axis)
        forward = [(i, (i + 1) % count) for i in range(count)]
        backward = [(target, source) for source, target in forward]
        low = lax.ppermute(
            lax.slice_in_dim(block, block.shape[dim] - width, None, axis=dim), axis, forward
        )
        high = lax.ppermute(lax.slice_in_dim(block, 0, width, axis=dim), axis, backward)
        block = jnp.concatenate([low, block, high], axis=dim)
    return block


def on_device(
    cell_counts,
    grid_offset,
    fraction,
    species,
    species_density,
    species_pair,
    species_embed,
    species_charge,
):
    cells_x, cells_y, cells_z, components, slots = fraction.shape
    cells = (cells_x, cells_y, cells_z)
    gx, gy, gz = (lax.axis_size(name) for name in ("gx", "gy", "gz"))
    devices = gx * gy * gz
    assert cells_x == gz and slots == 128
    lx, ly, lz = cells_x * gx * PPC, cells_y * gy * PPC, cells_z * gz * PPC
    assert lz % devices == 0
    modes = lz // devices
    yl = cells_y * PPC
    relayout = modes <= 128 and yl % max(1, 128 // modes) == 0

    table = jnp.stack(
        [
            species_density,
            species_pair,
            species_embed,
            species_charge,
            jnp.exp(jnp.log(species_density) * (1.0 / 3.0)),
            1.0 / (species_pair * species_pair),
            -3.0 * species_density / (species_pair * species_pair),
        ]
    )
    slot_index = lax.broadcasted_iota(jnp.int32, species.shape, 3)
    alive = slot_index < cell_counts[..., None]
    kind = jnp.where(alive, species.astype(F32), -1.0)[:, :, :, None, :]
    offsets = grid_offset.astype(F32)
    positions = (offsets + 0.5 + fraction) / PPC

    atoms = jnp.concatenate([offsets, fraction, kind, kind], axis=3)
    atoms = lax.all_to_all(atoms, "gz", split_axis=0, concat_axis=0, tiled=True)
    basis_x, basis_z = real_basis(lx), real_basis(lz)
    x_pair, xt_pair, z_pair = table_pair(basis_x), table_pair(basis_x.T), table_pair(basis_z)
    y_pair = table_pair(np.kron(real_basis(ly), np.eye(modes)))
    lines = make_spread(gz, cells_y, cells_z, slots, lz, devices, relayout)(atoms, table, *z_pair)
    if not relayout:
        lines = lines.reshape(yl, PPC, devices, modes).transpose(2, 1, 0, 3)
        lines = lines.reshape(devices, PPC, yl * modes)
    planes = lax.all_to_all(lines, ("gx", "gy", "gz"), split_axis=0, concat_axis=0, tiled=True)

    ext = padded(
        jnp.concatenate([positions, kind], axis=3), (("gz", 2), ("gy", 1), ("gx", 0)), 1
    )
    density, slope = make_density(cells, slots)(ext, table)
    slope_ext = padded(slope, (("gz", 2), ("gy", 1), ("gx", 0)), 1)

    width = ly * modes
    lane = lax.broadcasted_iota(jnp.int32, (1, width), 1)
    rank = lax.axis_index(("gx", "gy", "gz"))
    green = green_factor(
        signed_modes(lax.broadcasted_iota(jnp.int32, (lx, 1), 0), lx),
        signed_modes(lane // modes, ly),
        signed_modes(rank * modes + lane % modes, lz),
        lx,
        ly,
        lz,
    )
    planes = make_planes(gx, gy, gz, yl * modes, lx, width)(
        planes, *x_pair, *xt_pair, *y_pair, green
    )
    lines = lax.all_to_all(planes, ("gx", "gy", "gz"), split_axis=0, concat_axis=0, tiled=True)
    if not relayout:
        lines = lines.reshape(devices, PPC, yl, modes).transpose(2, 1, 0, 3)
        lines = lines.reshape(yl * PPC, lz)

    eam_force = make_force(cells, slots)(ext, slope_ext, table)

    electric = make_sample(gz, cells_y, cells_z, slots, lz, devices, relayout)(
        lines, atoms, table, *z_pair
    )
    electric = lax.all_to_all(electric, "gz", split_axis=0, concat_axis=0, tiled=True)
    forces = jnp.where(alive[:, :, :, None, :], eam_force + COUPLING * electric, 0.0)
    return (forces, density)


def solution(mesh):
    return jax.shard_map(
        on_device,
        mesh=mesh,
        in_specs=(
            P("gx", "gy", "gz"),
            P("gx", "gy", "gz", None, None),
            P("gx", "gy", "gz", None, None),
            P("gx", "gy", "gz", None),
            P(),
            P(),
            P(),
            P(),
        ),
        out_specs=(P("gx", "gy", "gz", None, None), P("gx", "gy", "gz", None)),
        check_vma=False,
    )
```

```python
import math

import ml_dtypes
import numpy as np

import jax
import jax.numpy as jnp
from jax import lax
from jax.experimental import pallas as pl
from jax.experimental.pallas import tpu as pltpu
from jax.sharding import PartitionSpec as P


NSPEC = 2
PPC = 16
EWALD_SPLIT = 0.7
COUPLING = 8.0
F32 = jnp.float32
BF16 = jnp.bfloat16
VMEM = pl.BlockSpec(memory_space=pltpu.VMEM)
SMEM = pl.BlockSpec(memory_space=pltpu.SMEM)
NN = (((1,), (0,)), ((), ()))
NT = (((1,), (1,)), ((), ()))
PARAMS = pltpu.CompilerParams(vmem_limit_bytes=56 * 1024 * 1024)


def split2(values):
    high = values.astype(BF16)
    return high, (values - high.astype(F32)).astype(BF16)


def split3(values):
    high = values.astype(BF16).astype(F32)
    rest = values - high
    middle = rest.astype(BF16).astype(F32)
    return high, middle, (rest - middle).astype(BF16).astype(F32)


def dot(left, right, dims):
    return lax.dot_general(left, right, dims, preferred_element_type=F32)


def dot3(left, right, dims):
    return (
        dot(left[0], right[0], dims) + dot(left[0], right[1], dims) + dot(left[1], right[0], dims)
    )


def by_kind(kind, table, column):
    result = jnp.zeros(kind.shape, F32)
    for kind_index in range(NSPEC):
        result = jnp.where(kind == float(kind_index), table[column, kind_index], result)
    return result


def real_basis(length):
    rows = np.arange(length)[:, None]
    points = np.arange(length)[None, :]
    half = length // 2
    waves = np.where(rows <= half, rows, length - rows)
    angle = 2.0 * np.pi * ((waves * points) % length) / length
    basis = np.where(rows <= half, np.cos(angle), np.sin(angle)) * math.sqrt(2.0 / length)
    basis[0] *= math.sqrt(0.5)
    basis[half] *= math.sqrt(0.5)
    return basis


def table_pair(values):
    values = values.astype(np.float32)
    high = values.astype(ml_dtypes.bfloat16)
    low = (values - high.astype(np.float32)).astype(ml_dtypes.bfloat16)
    return jnp.asarray(high), jnp.asarray(low)


def signed_modes(indices, total):
    return jnp.where(2 * indices >= total, indices - total, indices)


def green_factor(modes_x, modes_y, modes_z, length_x, length_y, length_z):
    wave_x = modes_x.astype(F32) * (2.0 * math.pi / length_x)
    wave_y = modes_y.astype(F32) * (2.0 * math.pi / length_y)
    wave_z = modes_z.astype(F32) * (2.0 * math.pi / length_z)
    squared = wave_x * wave_x + wave_y * wave_y + wave_z * wave_z
    anchor = (modes_x == 0) & (modes_y == 0) & (modes_z == 0)
    safe_square = jnp.where(anchor, 1.0, squared)
    return jnp.where(
        anchor,
        0.0,
        4.0 * math.pi * jnp.exp(-squared / (4.0 * EWALD_SPLIT * EWALD_SPLIT)) / safe_square,
    )


def chunk_transpose(tiles, chunk):
    tiles = list(tiles)
    count = len(tiles)
    width = tiles[0].shape[-1]
    lane_chunk = lax.broadcasted_iota(jnp.int32, tiles[0].shape, 1) // chunk
    bit = 1
    while bit < count:
        keep = (lane_chunk & bit) == 0
        for low in range(count):
            if low & bit:
                continue
            first, second = tiles[low], tiles[low | bit]
            tiles[low] = jnp.where(keep, first, pltpu.roll(second, bit * chunk, 1))
            tiles[low | bit] = jnp.where(keep, pltpu.roll(first, width - bit * chunk, 1), second)
        bit *= 2
    return tiles


def point_weights(offset_row, fraction_row):
    points = lax.broadcasted_iota(jnp.int32, (PPC, offset_row.shape[-1]), 0).astype(F32)
    lower = points == offset_row
    upper = points == offset_row + 1.0
    weights = jnp.where(lower, 1.0 - fraction_row, jnp.where(upper, fraction_row, 0.0))
    slopes = jnp.where(lower, -1.0, jnp.where(upper, 1.0, 0.0))
    return weights, slopes


def make_spread(parts, cells_y, cells_z, slots, lz, devices, relayout):
    columns = parts * cells_z
    modes = lz // devices
    yl = cells_y * PPC
    rows = PPC * PPC

    def kernel(atoms, table, basis_hi, basis_lo, out, plane_hi, plane_lo, line_hi, line_lo):
        line_hi[...] = jnp.zeros(line_hi.shape, BF16)
        line_lo[...] = jnp.zeros(line_lo.shape, BF16)
        basis = (basis_hi[...], basis_lo[...])
        pieces = []
        for cy in range(cells_y):
            for column in range(columns):
                cell = atoms[column // cells_z, cy, column % cells_z]
                weights = [point_weights(cell[d : d + 1], cell[3 + d : 4 + d])[0] for d in range(3)]
                along_x = weights[0] * by_kind(cell[6:7], table, 3)
                plane = jnp.concatenate(
                    [weights[1][y : y + 1] * along_x for y in range(PPC)], axis=0
                )
                lanes = pl.ds(column * slots, slots)
                points = pl.ds(column * PPC, PPC)
                plane_hi[:, lanes], plane_lo[:, lanes] = split2(plane)
                line_hi[points, lanes], line_lo[points, lanes] = split2(weights[2])
            brick = dot3(
                (plane_hi[...], plane_lo[...]), (line_hi[...], line_lo[...]), NT
            )
            pieces.append(dot3(split2(brick), basis, NT))
        if not relayout:
            for cy in range(cells_y):
                out[pl.ds(cy * rows, rows), :] = pieces[cy]
            return
        chunks = 128 // modes
        for tile in range(lz // 128):
            for group in range(yl // chunks):
                tiles = []
                for y in range(group * chunks, (group + 1) * chunks):
                    start = (y % PPC) * PPC
                    tiles.append(
                        pieces[y // PPC][start : start + PPC, tile * 128 : tile * 128 + 128]
                    )
                for chunk, value in enumerate(chunk_transpose(tiles, modes)):
                    out[tile * chunks + chunk, :, pl.ds(group * 128, 128)] = value

    if relayout:
        shape = (devices, PPC, yl * modes)
    else:
        shape = (cells_y * rows, lz)
    return pl.pallas_call(
        kernel,
        out_shape=jax.ShapeDtypeStruct(shape, F32),
        in_specs=[VMEM, SMEM, VMEM, VMEM],
        out_specs=VMEM,
        scratch_shapes=[
            pltpu.VMEM((rows, columns * slots), BF16),
            pltpu.VMEM((rows, columns * slots), BF16),
            pltpu.VMEM((lz, columns * slots), BF16),
            pltpu.VMEM((lz, columns * slots), BF16),
        ],
        compiler_params=PARAMS,
        name="spread",
    )


def make_planes(gx, gy, gz, lanes, lx, width):
    def kernel(data, x_hi, x_lo, xt_hi, xt_lo, y_hi, y_lo, green, out, grid):
        for a in range(gx):
            for b in range(gy):
                for c in range(gz):
                    grid[pl.ds((a * gz + c) * PPC, PPC), pl.ds(b * lanes, lanes)] = data[
                        (a * gy + b) * gz + c
                    ]
        along_y = (y_hi[...], y_lo[...])
        value = dot3((x_hi[...], x_lo[...]), split2(grid[...]), NN)
        value = dot3(split2(value), along_y, NT) * green[...]
        value = dot3(split2(value), along_y, NN)
        value = dot3((xt_hi[...], xt_lo[...]), split2(value), NN)
        for a in range(gx):
            for b in range(gy):
                for c in range(gz):
                    start = (a * gz + c) * PPC
                    out[(a * gy + b) * gz + c] = value[
                        start : start + PPC, b * lanes : (b + 1) * lanes
                    ]

    return pl.pallas_call(
        kernel,
        out_shape=jax.ShapeDtypeStruct((gx * gy * gz, PPC, lanes), F32),
        in_specs=[VMEM] * 8,
        out_specs=VMEM,
        scratch_shapes=[pltpu.VMEM((lx, width), F32)],
        compiler_params=PARAMS,
        name="planes",
    )


def make_sample(parts, cells_y, cells_z, slots, lz, devices, relayout):
    columns = parts * cells_z
    modes = lz // devices
    yl = cells_y * PPC
    rows = PPC * PPC

    def kernel(
        data, atoms, short, dens, table, basis_hi, basis_lo, out, lines, line_hi, line_lo
    ):
        if relayout:
            chunks = 128 // modes
            for tile in range(lz // 128):
                for group in range(yl // chunks):
                    tiles = [
                        data[tile * chunks + chunk, :, pl.ds(group * 128, 128)]
                        for chunk in range(chunks)
                    ]
                    for index, value in enumerate(chunk_transpose(tiles, modes)):
                        lines[
                            pl.ds((group * chunks + index) * PPC, PPC), pl.ds(tile * 128, 128)
                        ] = value
        else:
            lines[...] = data[...]
        line_hi[...] = jnp.zeros(line_hi.shape, BF16)
        line_lo[...] = jnp.zeros(line_lo.shape, BF16)
        basis = (basis_hi[...], basis_lo[...])
        for cy in range(cells_y):
            brick = split2(dot3(split2(lines[pl.ds(cy * rows, rows), :]), basis, NN))
            for column in range(columns):
                cell = atoms[column // cells_z, cy, column % cells_z]
                pairs = [point_weights(cell[d : d + 1], cell[3 + d : 4 + d]) for d in range(3)]
                (wx, sx), (wy, sy), (wz, sz) = pairs
                points = pl.ds(column * PPC, PPC)
                high, low = split2(wz)
                line_hi[column, points, pl.ds(0, slots)] = high
                line_hi[column, points, pl.ds(slots, slots)] = sz.astype(BF16)
                line_lo[column, points, :] = low
                both = dot(brick[0], line_hi[column], NN) + dot(brick[1], line_hi[column], NN)
                plain = both[:, :slots] + dot(brick[0], line_lo[column], NN)
                tilted = both[:, slots:]
                force_x = jnp.zeros((PPC, slots), F32)
                force_y = jnp.zeros((PPC, slots), F32)
                force_z = jnp.zeros((PPC, slots), F32)
                for y in range(PPC):
                    block = plain[y * PPC : (y + 1) * PPC]
                    force_x += wy[y : y + 1] * block
                    force_y += sy[y : y + 1] * block
                    force_z += wy[y : y + 1] * tilted[y * PPC : (y + 1) * PPC]
                charge = -COUPLING * by_kind(cell[6:7], table, 3)
                here = pl.ds(column, 1)
                result = [
                    charge * jnp.sum(force * weight, axis=0, keepdims=True)
                    + short[d, cy, here, :]
                    for d, (force, weight) in enumerate(
                        ((force_x, sx), (force_y, wx), (force_z, wx))
                    )
                ]
                result = [jnp.where(cell[6:7] >= 0.0, value, 0.0) for value in result]
                result.append(dens[cy, here, :])
                out[column // cells_z, cy, column % cells_z] = jnp.concatenate(result, axis=0)

    return pl.pallas_call(
        kernel,
        out_shape=jax.ShapeDtypeStruct((parts, cells_y, cells_z, 4, slots), F32),
        in_specs=[VMEM, VMEM, VMEM, VMEM, SMEM, VMEM, VMEM],
        out_specs=VMEM,
        scratch_shapes=[
            pltpu.VMEM((cells_y * rows, lz), F32),
            pltpu.VMEM((columns, lz, 2 * slots), BF16),
            pltpu.VMEM((columns, lz, slots), BF16),
        ],
        compiler_params=PARAMS,
        name="sample",
    )


WIDE = ((0, 0), (1, 0), (0, 1), (1, 1), (2, 0), (0, 2))
SHORT = WIDE[:4]


def piece_rows(values, order, side):
    pieces = split3(values)
    return jnp.concatenate([pieces[entry[side]] for entry in order], axis=0)


def channel(block, y, nz, index):
    return block[pl.ds(y * nz * 4 + index, nz, stride=4), :]


def row_positions(block, x, y, sy, nz):
    pos_x = channel(block, y, nz, 0) + (x - 1.0)
    pos_y = channel(block, y, nz, 1) + (y - 0.5 * (sy - 1))
    return pos_x, pos_y, channel(block, y, nz, 2)


def same_slot(slots):
    return lax.broadcasted_iota(jnp.int32, (slots, slots), 0) == lax.broadcasted_iota(
        jnp.int32, (slots, slots), 1
    )


def make_density(cells_y, nz, slots):
    sy = cells_y + 2
    own = cells_y * nz
    total = 3 * sy * nz

    def kernel(low, mid, high, table, density, slope, feature, own_feature, right, left, sums):
        feature[...] = jnp.zeros(feature.shape, F32)
        own_feature[...] = jnp.zeros(own_feature.shape, F32)
        for x, block in enumerate((low, mid, high)):
            for y in range(sy):
                pos = row_positions(block, x, y, sy, nz)
                square = pos[0] * pos[0] + pos[1] * pos[1] + pos[2] * pos[2]
                scale = by_kind(channel(block, y, nz, 3), table, 4)
                base = (x * sy + y) * nz * 8
                feature[pl.ds(base, nz, stride=8), :] = scale * (1.0 - square)
                for d in range(3):
                    feature[pl.ds(base + 1 + d, nz, stride=8), :] = 2.0 * scale * pos[d]
                feature[pl.ds(base + 4, nz, stride=8), :] = -scale
                if x == 1 and 1 <= y <= cells_y:
                    for dz in range(3):
                        across = pos[2] - (dz - 1.0)
                        square = pos[0] * pos[0] + pos[1] * pos[1] + across * across
                        base = (dz * own + (y - 1) * nz) * 8
                        rows = (jnp.ones_like(square), pos[0], pos[1], across, square)
                        for k, value in enumerate(rows):
                            own_feature[pl.ds(base + k, nz, stride=8), :] = value

        def fill_right(n, carry):
            right[n] = piece_rows(feature[pl.ds(n * 8, 8), :], WIDE, 0).astype(BF16)
            return carry

        def fill_left(n, carry):
            left[n] = piece_rows(own_feature[pl.ds(n * 8, 8), :], WIDE, 1).T.astype(BF16)
            return carry

        lax.fori_loop(0, total, fill_right, 0, unroll=8)
        lax.fori_loop(0, 3 * own, fill_left, 0, unroll=8)
        same = same_slot(slots)
        lane = lax.broadcasted_iota(jnp.int32, (slots, 128), 1)
        sums[...] = jnp.zeros(sums.shape, F32)

        def one_cell(n, carry):
            y, z = n // nz, n % nz
            weight = jnp.maximum(dot(left[own + n], right[(sy + y + 1) * nz + z], NN), 0.0)
            weight = jnp.where(same, 0.0, weight)
            total_sum = weight * weight * weight
            for dz in range(3):
                zz = (z + (dz - 1 + nz)) % nz
                lhs = left[dz * own + n]
                near = [(dx * sy + y + dy) * nz + zz for dx in range(3) for dy in range(3)]
                if dz == 1:
                    near.pop(4)
                while near:
                    pair, near = near[:2], near[2:]
                    rhs = [right[index] for index in pair]
                    rhs = jnp.concatenate(rhs, axis=1) if len(rhs) > 1 else rhs[0]
                    weight = jnp.maximum(dot(lhs, rhs, NN), 0.0)
                    cube = weight * weight * weight
                    for part in range(len(pair)):
                        total_sum = total_sum + cube[:, part * slots : (part + 1) * slots]
            column = jnp.sum(total_sum, axis=1, keepdims=True)
            sums[...] = jnp.where(lane == n, column, sums[...])
            return carry

        lax.fori_loop(0, own, one_cell, 0, unroll=2)
        rows = sums[...].T
        for y in range(cells_y):
            kind = channel(mid, y + 1, nz, 3)
            value = jnp.where(kind >= 0.0, rows[y * nz : (y + 1) * nz], 0.0)
            density[y] = value
            slope[y] = -by_kind(kind, table, 2) / (2.0 * jnp.sqrt(1.0 + value))

    shape = jax.ShapeDtypeStruct((cells_y, nz, slots), F32)
    return pl.pallas_call(
        kernel,
        out_shape=(shape, shape),
        in_specs=[VMEM, VMEM, VMEM, SMEM],
        out_specs=(VMEM, VMEM),
        scratch_shapes=[
            pltpu.VMEM((total * 8, slots), F32),
            pltpu.VMEM((3 * own * 8, slots), F32),
            pltpu.VMEM((total, 48, slots), BF16),
            pltpu.VMEM((3 * own, slots, 48), BF16),
            pltpu.VMEM((slots, 128), F32),
        ],
        compiler_params=PARAMS,
        cost_estimate=pl.CostEstimate(
            flops=own * 27 * slots * slots * 40, bytes_accessed=total * slots * 16, transcendentals=0
        ),
        name="density",
    )


def make_force(cells_y, nz, slots):
    sy = cells_y + 2
    own = cells_y * nz
    total = 3 * sy * nz
    chunk = 64

    def kernel(
        low, mid, high, slope_low, slope_mid, slope_high, table, out,
        feature, extra, own_feature, own_extra, place, right, right_extra, left, left_extra,
        sums,
    ):
        for ref in (feature, extra, own_feature, own_extra):
            ref[...] = jnp.zeros(ref.shape, F32)
        blocks = zip((low, mid, high), (slope_low, slope_mid, slope_high))
        for x, (block, slopes) in enumerate(blocks):
            for y in range(sy):
                pos = row_positions(block, x, y, sy, nz)
                square = pos[0] * pos[0] + pos[1] * pos[1] + pos[2] * pos[2]
                kind = channel(block, y, nz, 3)
                scale = by_kind(kind, table, 1)
                steep = slopes[y] * by_kind(kind, table, 5)
                mild = by_kind(kind, table, 6)
                base = (x * sy + y) * nz * 8
                feature[pl.ds(base, nz, stride=8), :] = scale * (1.0 - square)
                for d in range(3):
                    feature[pl.ds(base + 1 + d, nz, stride=8), :] = 2.0 * scale * pos[d]
                    place[pl.ds(base + d, nz, stride=8), :] = pos[d]
                feature[pl.ds(base + 4, nz, stride=8), :] = -scale
                extra[pl.ds(base, nz, stride=8), :] = steep
                extra[pl.ds(base + 1, nz, stride=8), :] = mild
                if x == 1 and 1 <= y <= cells_y:
                    base = (y - 1) * nz * 8
                    own_extra[pl.ds(base, nz, stride=8), :] = mild
                    own_extra[pl.ds(base + 1, nz, stride=8), :] = steep
                    for dz in range(3):
                        across = pos[2] - (dz - 1.0)
                        square = pos[0] * pos[0] + pos[1] * pos[1] + across * across
                        base = (dz * own + (y - 1) * nz) * 8
                        rows = (1.0, pos[0], pos[1], across, square)
                        for k, value in enumerate(rows):
                            own_feature[pl.ds(base + k, nz, stride=8), :] = scale * value

        def fill_right(n, carry):
            rows = pl.ds(n * 8, 8)
            right[n] = piece_rows(feature[rows, :], WIDE, 0).astype(BF16)
            right_extra[n] = piece_rows(extra[rows, :], SHORT, 0).astype(BF16)
            return carry

        def fill_left(n, carry):
            left[n] = piece_rows(own_feature[pl.ds(n * 8, 8), :], WIDE, 1).T.astype(BF16)
            return carry

        def fill_left_extra(n, carry):
            left_extra[n] = piece_rows(own_extra[pl.ds(n * 8, 8), :], SHORT, 1).T.astype(BF16)
            return carry

        lax.fori_loop(0, total, fill_right, 0, unroll=8)
        lax.fori_loop(0, 3 * own, fill_left, 0, unroll=8)
        lax.fori_loop(0, own, fill_left_extra, 0, unroll=8)
        same = same_slot(slots)
        lane = lax.broadcasted_iota(jnp.int32, (slots, 128), 1)
        sums[...] = jnp.zeros(sums.shape, F32)

        def one_cell(n, carry):
            y, z = n // nz, n % nz
            for start in range(0, slots, chunk):
                rows = pl.ds(start, chunk)
                lhs_extra = left_extra[n, rows, :]
                parts = [jnp.zeros((chunk, slots), F32) for _ in range(4)]
                for dz in range(3):
                    zz = (z + (dz - 1 + nz)) % nz
                    lhs = left[dz * own + n, rows, :]
                    near = [(dx * sy + y + dy) * nz + zz for dx in range(3) for dy in range(3)]
                    if dz == 1:
                        near.append(near.pop(4))
                    for index in range(0, 9, 2):
                        pair = near[index : index + 2]
                        rhs = [right[cell] for cell in pair]
                        rhs_extra = [right_extra[cell] for cell in pair]
                        if len(pair) > 1:
                            rhs = [jnp.concatenate(rhs, axis=1)]
                            rhs_extra = [jnp.concatenate(rhs_extra, axis=1)]
                        weight = jnp.maximum(dot(lhs, rhs[0], NN), 0.0)
                        if dz == 1 and index == 8:
                            weight = jnp.where(same[start : start + chunk], 0.0, weight)
                        value = (weight * dot(lhs_extra, rhs_extra[0], NN) - 2.0) * weight
                        for k, cell in enumerate(pair):
                            tile = value[:, k * slots : (k + 1) * slots]
                            parts[3] = parts[3] + tile
                            for d in range(3):
                                there = place[pl.ds(cell * 8 + d, 1), :]
                                if d == 2 and dz != 1:
                                    there = there + (dz - 1.0)
                                parts[d] = parts[d] + tile * there
                for d in range(4):
                    column = jnp.sum(parts[d], axis=1, keepdims=True)
                    sums[d, rows, :] = jnp.where(
                        lane[start : start + chunk] == n, column, sums[d, rows, :]
                    )
            return carry

        lax.fori_loop(0, own, one_cell, 0, unroll=2)
        rows = [sums[d].T for d in range(4)]
        for y in range(cells_y):
            pos = row_positions(mid, 1, y + 1, sy, nz)
            part = slice(y * nz, (y + 1) * nz)
            for d in range(3):
                out[d, y] = 2.0 * (rows[d][part] - pos[d] * rows[3][part])

    return pl.pallas_call(
        kernel,
        out_shape=jax.ShapeDtypeStruct((3, cells_y, nz, slots), F32),
        in_specs=[VMEM] * 6 + [SMEM],
        out_specs=VMEM,
        scratch_shapes=[
            pltpu.VMEM((total * 8, slots), F32),
            pltpu.VMEM((total * 8, slots), F32),
            pltpu.VMEM((3 * own * 8, slots), F32),
            pltpu.VMEM((own * 8, slots), F32),
            pltpu.VMEM((total * 8, slots), F32),
            pltpu.VMEM((total, 48, slots), BF16),
            pltpu.VMEM((total, 32, slots), BF16),
            pltpu.VMEM((3 * own, slots, 48), BF16),
            pltpu.VMEM((own, slots, 32), BF16),
            pltpu.VMEM((4, slots, 128), F32),
        ],
        compiler_params=PARAMS,
        cost_estimate=pl.CostEstimate(
            flops=own * 27 * slots * slots * 100,
            bytes_accessed=total * slots * 16,
            transcendentals=0,
        ),
        name="force",
    )


def shifted(axis, count):
    up = [(i, (i + 1) % count) for i in range(count)]
    down = [(target, source) for source, target in up]
    return lambda part: lax.ppermute(part, axis, up), lambda part: lax.ppermute(part, axis, down)


def halo(block, gx, gy, gz):
    up, down = shifted("gy", gy)
    if gy == 2 and block.shape[0] == 2:
        other = up(block)
        low, high = other[-1:], other[:1]
    else:
        low, high = up(block[-1:]), down(block[:1])
    middle = jnp.concatenate([low, block, high], axis=0)
    up, down = shifted(("gx", "gz"), gx * gz)
    low = up(middle)
    high = down(middle)
    return low, middle, high


def on_device(
    cell_counts,
    grid_offset,
    fraction,
    species,
    species_density,
    species_pair,
    species_embed,
    species_charge,
):
    cells_x, cells_y, cells_z, _, slots = fraction.shape
    gx, gy, gz = (lax.axis_size(name) for name in ("gx", "gy", "gz"))
    devices = gx * gy * gz
    assert cells_x == gz and slots == 128
    lx, ly, lz = cells_x * gx * PPC, cells_y * gy * PPC, cells_z * gz * PPC
    assert lz % devices == 0
    modes = lz // devices
    yl = cells_y * PPC
    relayout = modes <= 128 and yl % max(1, 128 // modes) == 0

    table = jnp.stack(
        [
            species_density,
            species_pair,
            species_embed,
            species_charge,
            jnp.exp(jnp.log(species_density) * (1.0 / 3.0)),
            1.0 / (species_pair * species_pair),
            -3.0 * species_density / (species_pair * species_pair),
        ]
    )
    slot_index = lax.broadcasted_iota(jnp.int32, species.shape, 3)
    alive = slot_index < cell_counts[..., None]
    kind = jnp.where(alive, species.astype(F32), -1.0)[:, :, :, None, :]
    offsets = grid_offset.astype(F32)

    atoms = jnp.concatenate([offsets, fraction, kind, kind], axis=3)
    atoms = lax.all_to_all(atoms, "gz", split_axis=0, concat_axis=0, tiled=True)
    basis_x, basis_z = real_basis(lx), real_basis(lz)
    x_pair, xt_pair, z_pair = table_pair(basis_x), table_pair(basis_x.T), table_pair(basis_z)
    y_pair = table_pair(np.kron(real_basis(ly), np.eye(modes)))
    spread = make_spread(gz, cells_y, cells_z, slots, lz, devices, relayout)
    lines = spread(atoms, table, *z_pair)
    if not relayout:
        lines = lines.reshape(yl, PPC, devices, modes).transpose(2, 1, 0, 3)
        lines = lines.reshape(devices, PPC, yl * modes)
    planes = lax.all_to_all(lines, ("gx", "gy", "gz"), split_axis=0, concat_axis=0, tiled=True)

    nz = gz * cells_z
    place = (atoms[:, :, :, 0:3] + 0.5 + atoms[:, :, :, 3:6]) / PPC - 0.5
    place = jnp.concatenate([place, atoms[:, :, :, 6:7]], axis=3)
    place = place.transpose(1, 0, 2, 3, 4).reshape(cells_y, nz, 4, slots)
    near = [part.reshape((cells_y + 2) * nz * 4, slots) for part in halo(place, gx, gy, gz)]
    density, slope = make_density(cells_y, nz, slots)(*near, table)
    near_slopes = halo(slope, gx, gy, gz)

    width = ly * modes
    lane = lax.broadcasted_iota(jnp.int32, (1, width), 1)
    rank = lax.axis_index(("gx", "gy", "gz"))
    green = green_factor(
        signed_modes(lax.broadcasted_iota(jnp.int32, (lx, 1), 0), lx),
        signed_modes(lane // modes, ly),
        signed_modes(rank * modes + lane % modes, lz),
        lx,
        ly,
        lz,
    )
    planes = make_planes(gx, gy, gz, yl * modes, lx, width)(
        planes, *x_pair, *xt_pair, *y_pair, green
    )
    lines = lax.all_to_all(planes, ("gx", "gy", "gz"), split_axis=0, concat_axis=0, tiled=True)
    if not relayout:
        lines = lines.reshape(devices, PPC, yl, modes).transpose(2, 1, 0, 3)
        lines = lines.reshape(yl * PPC, lz)

    short = make_force(cells_y, nz, slots)(*near, *near_slopes, table)
    result = make_sample(gz, cells_y, cells_z, slots, lz, devices, relayout)(
        lines, atoms, short, density, table, *z_pair
    )
    result = lax.all_to_all(result, "gz", split_axis=0, concat_axis=0, tiled=True)
    return (result[:, :, :, 0:3], result[:, :, :, 3])


def solution(mesh):
    return jax.shard_map(
        on_device,
        mesh=mesh,
        in_specs=(
            P("gx", "gy", "gz"),
            P("gx", "gy", "gz", None, None),
            P("gx", "gy", "gz", None, None),
            P("gx", "gy", "gz", None),
            P(),
            P(),
            P(),
            P(),
        ),
        out_specs=(P("gx", "gy", "gz", None, None), P("gx", "gy", "gz", None)),
        check_vma=False,
    )
```

```python
import math

import ml_dtypes
import numpy as np

import jax
import jax.numpy as jnp
from jax import lax
from jax.experimental import pallas as pl
from jax.experimental.pallas import tpu as pltpu
from jax.sharding import PartitionSpec as P


NSPEC = 2
PPC = 16
EWALD_SPLIT = 0.7
COUPLING = 8.0
F32 = jnp.float32
BF16 = jnp.bfloat16
VMEM = pl.BlockSpec(memory_space=pltpu.VMEM)
SMEM = pl.BlockSpec(memory_space=pltpu.SMEM)
ANY = pl.BlockSpec(memory_space=pl.ANY)
NN = (((1,), (0,)), ((), ()))
NT = (((1,), (1,)), ((), ()))
PARAMS = pltpu.CompilerParams(vmem_limit_bytes=56 * 1024 * 1024)


def near_core(values):
    return pltpu.with_memory_space_constraint(values, pltpu.VMEM)


def split2(values):
    high = values.astype(BF16)
    return high, (values - high.astype(F32)).astype(BF16)


def split3(values):
    high = values.astype(BF16).astype(F32)
    rest = values - high
    middle = rest.astype(BF16).astype(F32)
    return high, middle, (rest - middle).astype(BF16).astype(F32)


def dot(left, right, dims):
    return lax.dot_general(left, right, dims, preferred_element_type=F32)


def dot3(left, right, dims):
    return (
        dot(left[0], right[0], dims) + dot(left[0], right[1], dims) + dot(left[1], right[0], dims)
    )


def by_kind(kind, table, empty=0.0):
    result = jnp.full(kind.shape, empty, F32)
    for kind_index in range(NSPEC):
        result = jnp.where(kind == float(kind_index), table[kind_index], result)
    return result


def real_basis(length):
    rows = np.arange(length)[:, None]
    points = np.arange(length)[None, :]
    half = length // 2
    waves = np.where(rows <= half, rows, length - rows)
    angle = 2.0 * np.pi * ((waves * points) % length) / length
    basis = np.where(rows <= half, np.cos(angle), np.sin(angle)) * math.sqrt(2.0 / length)
    basis[0] *= math.sqrt(0.5)
    basis[half] *= math.sqrt(0.5)
    return basis


def table_pair(values):
    values = values.astype(np.float32)
    high = values.astype(ml_dtypes.bfloat16)
    low = (values - high.astype(np.float32)).astype(ml_dtypes.bfloat16)
    return jnp.asarray(np.stack([high, low]))


def signed_modes(indices, total):
    return jnp.where(2 * indices >= total, indices - total, indices)


def chunk_transpose(tiles, chunk):
    tiles = list(tiles)
    count = len(tiles)
    width = tiles[0].shape[-1]
    lane_chunk = lax.broadcasted_iota(jnp.int32, tiles[0].shape, 1) // chunk
    bit = 1
    while bit < count:
        keep = (lane_chunk & bit) == 0
        for low in range(count):
            if low & bit:
                continue
            first, second = tiles[low], tiles[low | bit]
            tiles[low] = jnp.where(keep, first, pltpu.roll(second, bit * chunk, 1))
            tiles[low | bit] = jnp.where(keep, pltpu.roll(first, width - bit * chunk, 1), second)
        bit *= 2
    return tiles


def point_weights(offset_row, fraction_row):
    points = lax.broadcasted_iota(jnp.int32, (PPC, offset_row.shape[-1]), 0).astype(F32)
    lower = points == offset_row
    upper = points == offset_row + 1.0
    weights = jnp.where(lower, 1.0 - fraction_row, jnp.where(upper, fraction_row, 0.0))
    slopes = jnp.where(lower, -1.0, jnp.where(upper, 1.0, 0.0))
    return weights, slopes


def make_spread(parts, cells_y, cells_z, slots, lz, devices, relayout):
    columns = parts * cells_z
    modes = lz // devices
    yl = cells_y * PPC
    rows = PPC * PPC

    tiles = lz // 128
    reach = columns // tiles

    def kernel(atoms, table, basis_any, out, plane, line_hi, line_lo, basis_ref, sem):
        fetch = pltpu.make_async_copy(basis_any, basis_ref, sem)
        fetch.start()
        line_hi[...] = jnp.zeros(line_hi.shape, BF16)
        line_lo[...] = jnp.zeros(line_lo.shape, BF16)
        pieces = []
        for cy in range(cells_y):
            brick = []
            for tile in range(tiles):
                for place in range(reach):
                    column = tile * reach + place
                    cell = atoms[column // cells_z, cy, :, column % cells_z, :]
                    weights = [
                        point_weights(cell[d : d + 1], cell[3 + d : 4 + d])[0] for d in range(3)
                    ]
                    along_x = weights[0] * by_kind(cell[6:7], table)
                    value = jnp.concatenate(
                        [weights[1][y : y + 1] * along_x for y in range(PPC)], axis=0
                    )
                    lanes = pl.ds(place * slots, slots)
                    points = pl.ds(place * PPC, PPC)
                    high, low = split2(value)
                    plane[tile, pl.ds(0, rows), lanes] = high
                    plane[tile, pl.ds(rows, rows), lanes] = low
                    high, low = split2(weights[2])
                    line_hi[tile, points, lanes] = high
                    line_lo[tile, points, lanes] = low
                wide = dot(plane[tile], line_hi[tile], NT)
                brick.append(
                    wide[:rows] + wide[rows:] + dot(plane[tile, pl.ds(0, rows), :], line_lo[tile], NT)
                )
            if cy == 0:
                fetch.wait()
            brick = jnp.concatenate(brick, axis=1)
            pieces.append(dot3(split2(brick), (basis_ref[0], basis_ref[1]), NT))
        if not relayout:
            for cy in range(cells_y):
                out[pl.ds(cy * rows, rows), :] = pieces[cy]
            return
        chunks = 128 // modes
        for tile in range(tiles):
            for group in range(yl // chunks):
                parts = []
                for y in range(group * chunks, (group + 1) * chunks):
                    start = (y % PPC) * PPC
                    parts.append(
                        pieces[y // PPC][start : start + PPC, tile * 128 : tile * 128 + 128]
                    )
                for chunk, value in enumerate(chunk_transpose(parts, modes)):
                    out[tile * chunks + chunk, :, pl.ds(group * 128, 128)] = value

    if relayout:
        shape = (devices, PPC, yl * modes)
    else:
        shape = (cells_y * rows, lz)
    return pl.pallas_call(
        kernel,
        out_shape=pltpu.VMEM(shape, F32),
        in_specs=[VMEM, SMEM, ANY],
        out_specs=VMEM,
        scratch_shapes=[
            pltpu.VMEM((tiles, 2 * rows, reach * slots), BF16),
            pltpu.VMEM((tiles, 128, reach * slots), BF16),
            pltpu.VMEM((tiles, 128, reach * slots), BF16),
            pltpu.VMEM((2, lz, lz), BF16),
            pltpu.SemaphoreType.DMA(()),
        ],
        compiler_params=PARAMS,
        name="spread",
    )


def make_planes(gx, gy, gz, lanes, lx, ly, lz):
    modes = lz // (gx * gy * gz)
    width = ly * modes
    sharp = -1.0 / (4.0 * EWALD_SPLIT * EWALD_SPLIT)

    def wave_square(indices, length):
        return jnp.square(signed_modes(indices, length).astype(F32) * (2.0 * math.pi / length))

    def kernel(rank, data, x_any, xt_any, y_any, out, grid, x_ref, xt_ref, y_ref, sems):
        fetches = [
            pltpu.make_async_copy(source, target, sems.at[index])
            for index, (source, target) in enumerate(
                ((x_any, x_ref), (y_any, y_ref), (xt_any, xt_ref))
            )
        ]
        for fetch in fetches:
            fetch.start()
        for a in range(gx):
            for b in range(gy):
                for c in range(gz):
                    grid[pl.ds((a * gz + c) * PPC, PPC), pl.ds(b * lanes, lanes)] = data[
                        (a * gy + b) * gz + c
                    ]
        lane = lax.broadcasted_iota(jnp.int32, (1, width), 1)
        across = wave_square(lane // modes, ly) + wave_square(rank[0] * modes + lane % modes, lz)
        along = wave_square(lax.broadcasted_iota(jnp.int32, (lx, 1), 0), lx)
        squared = along + across
        factor = (4.0 * math.pi * jnp.exp(along * sharp)) * jnp.exp(across * sharp)
        green = jnp.where(squared == 0.0, 0.0, factor / jnp.where(squared == 0.0, 1.0, squared))
        fetches[0].wait()
        value = dot3((x_ref[0], x_ref[1]), split2(grid[...]), NN)
        fetches[1].wait()
        value = dot3(split2(value), (y_ref[0], y_ref[1]), NT) * green
        value = dot3(split2(value), (y_ref[0], y_ref[1]), NN)
        fetches[2].wait()
        value = dot3((xt_ref[0], xt_ref[1]), split2(value), NN)
        for a in range(gx):
            for b in range(gy):
                for c in range(gz):
                    start = (a * gz + c) * PPC
                    out[(a * gy + b) * gz + c] = value[
                        start : start + PPC, b * lanes : (b + 1) * lanes
                    ]

    return pl.pallas_call(
        kernel,
        out_shape=pltpu.VMEM((gx * gy * gz, PPC, lanes), F32),
        in_specs=[SMEM, VMEM, ANY, ANY, ANY],
        out_specs=VMEM,
        scratch_shapes=[
            pltpu.VMEM((lx, width), F32),
            pltpu.VMEM((2, lx, lx), BF16),
            pltpu.VMEM((2, lx, lx), BF16),
            pltpu.VMEM((2, width, width), BF16),
            pltpu.SemaphoreType.DMA((3,)),
        ],
        compiler_params=PARAMS,
        name="planes",
    )


def make_sample(parts, cells_y, cells_z, slots, lz, devices, relayout):
    columns = parts * cells_z
    modes = lz // devices
    yl = cells_y * PPC
    rows = PPC * PPC

    reach = columns * 128 // lz

    def kernel(
        data, atoms, short, dens, table, basis_any, out, lines, line, basis_ref, sem
    ):
        fetch = pltpu.make_async_copy(basis_any, basis_ref, sem)
        fetch.start()
        if relayout:
            chunks = 128 // modes
            for tile in range(lz // 128):
                for group in range(yl // chunks):
                    tiles = [
                        data[tile * chunks + chunk, :, pl.ds(group * 128, 128)]
                        for chunk in range(chunks)
                    ]
                    for index, value in enumerate(chunk_transpose(tiles, modes)):
                        lines[
                            pl.ds((group * chunks + index) * PPC, PPC), pl.ds(tile * 128, 128)
                        ] = value
        else:
            lines[...] = data[...]
        line[...] = jnp.zeros(line.shape, BF16)
        fetch.wait()
        for cy in range(cells_y):
            brick = dot3(
                split2(lines[pl.ds(cy * rows, rows), :]), (basis_ref[0], basis_ref[1]), NN
            )
            for column in range(columns):
                if column % reach == 0:
                    start = column // reach * 128
                    high, low = split2(brick[:, start : start + 128])
                    wide = jnp.concatenate([high, low, high], axis=1)
                cell = atoms[column // cells_z, cy, :, column % cells_z, :]
                pairs = [point_weights(cell[d : d + 1], cell[3 + d : 4 + d]) for d in range(3)]
                (wx, sx), (wy, sy), (wz, sz) = pairs
                first = column % reach * PPC
                high, low = split2(wz)
                both = jnp.concatenate([high, sz.astype(BF16)], axis=1)
                line[column, pl.ds(first, PPC), :] = both
                line[column, pl.ds(128 + first, PPC), :] = both
                line[column, pl.ds(256 + first, PPC), pl.ds(0, slots)] = low
                both = dot(wide, line[column], NN)
                plain, tilted = both[:, :slots], both[:, slots:]
                force_x = jnp.zeros((PPC, slots), F32)
                force_y = jnp.zeros((PPC, slots), F32)
                force_z = jnp.zeros((PPC, slots), F32)
                for y in range(PPC):
                    block = plain[y * PPC : (y + 1) * PPC]
                    force_x += wy[y : y + 1] * block
                    force_y += sy[y : y + 1] * block
                    force_z += wy[y : y + 1] * tilted[y * PPC : (y + 1) * PPC]
                charge = -COUPLING * by_kind(cell[6:7], table)
                here = pl.ds(column, 1)
                result = [
                    charge * jnp.sum(force * weight, axis=0, keepdims=True)
                    + short[d, cy, here, :]
                    for d, (force, weight) in enumerate(
                        ((force_x, sx), (force_y, wx), (force_z, wx))
                    )
                ]
                result = [jnp.where(cell[6:7] >= 0.0, value, 0.0) for value in result]
                result.append(dens[cy, here, :])
                out[column // cells_z, cy, :, column % cells_z, :] = jnp.concatenate(result, axis=0)

    return pl.pallas_call(
        kernel,
        out_shape=pltpu.VMEM((parts, cells_y, 4, cells_z, slots), F32),
        in_specs=[VMEM, VMEM, VMEM, VMEM, SMEM, ANY],
        out_specs=VMEM,
        scratch_shapes=[
            pltpu.VMEM((cells_y * rows, lz), F32),
            pltpu.VMEM((columns, 384, 2 * slots), BF16),
            pltpu.VMEM((2, lz, lz), BF16),
            pltpu.SemaphoreType.DMA(()),
        ],
        compiler_params=PARAMS,
        name="sample",
    )


WIDE = ((0, 0), (1, 0), (0, 1), (1, 1), (2, 0), (0, 2))
SHORT = WIDE[:4]


def piece_rows(values, order, side):
    pieces = split3(values)
    return jnp.concatenate([pieces[entry[side]] for entry in order], axis=0)


def channel(block, y, nz, index):
    return block[pl.ds((y * 4 + index) * nz, nz), :]


def row_positions(block, x, y, sy, nz):
    pos_x = channel(block, y, nz, 0) + (x - 1.0)
    pos_y = channel(block, y, nz, 1) + (y - 0.5 * (sy - 1))
    return pos_x, pos_y, channel(block, y, nz, 2)


def same_slot(slots):
    return lax.broadcasted_iota(jnp.int32, (slots, slots), 0) == lax.broadcasted_iota(
        jnp.int32, (slots, slots), 1
    )


def make_density(cells_y, nz, slots):
    sy = cells_y + 2
    own = cells_y * nz
    total = 3 * sy * nz

    def kernel(
        low, mid, high, electrons, embed, density, slope, feature, own_feature, right, left, sums
    ):
        feature[...] = jnp.zeros(feature.shape, F32)
        own_feature[...] = jnp.zeros(own_feature.shape, F32)
        for x, block in enumerate((low, mid, high)):
            for y in range(sy):
                pos = row_positions(block, x, y, sy, nz)
                square = pos[0] * pos[0] + pos[1] * pos[1] + pos[2] * pos[2]
                kind = channel(block, y, nz, 3)
                scale = jnp.exp(jnp.log(by_kind(kind, electrons, 1.0)) * (1.0 / 3.0))
                scale = jnp.where(kind >= 0.0, scale, 0.0)
                base = (x * sy + y) * nz * 8
                feature[pl.ds(base, nz, stride=8), :] = scale * (1.0 - square)
                for d in range(3):
                    feature[pl.ds(base + 1 + d, nz, stride=8), :] = 2.0 * scale * pos[d]
                feature[pl.ds(base + 4, nz, stride=8), :] = -scale
                if x == 1 and 1 <= y <= cells_y:
                    for dz in range(3):
                        across = pos[2] - (dz - 1.0)
                        square = pos[0] * pos[0] + pos[1] * pos[1] + across * across
                        base = (dz * own + (y - 1) * nz) * 8
                        rows = (jnp.ones_like(square), pos[0], pos[1], across, square)
                        for k, value in enumerate(rows):
                            own_feature[pl.ds(base + k, nz, stride=8), :] = value

        def fill_right(n, carry):
            right[n] = piece_rows(feature[pl.ds(n * 8, 8), :], WIDE, 0).astype(BF16)
            return carry

        def fill_left(n, carry):
            left[n] = piece_rows(own_feature[pl.ds(n * 8, 8), :], WIDE, 1).T.astype(BF16)
            return carry

        lax.fori_loop(0, total, fill_right, 0, unroll=8)
        lax.fori_loop(0, 3 * own, fill_left, 0, unroll=8)
        same = same_slot(slots)
        lane = lax.broadcasted_iota(jnp.int32, (slots, 128), 1)
        sums[...] = jnp.zeros(sums.shape, F32)

        def one_cell(n, carry):
            y, z = n // nz, n % nz
            weight = jnp.maximum(dot(left[own + n], right[(sy + y + 1) * nz + z], NN), 0.0)
            weight = jnp.where(same, 0.0, weight)
            total_sum = weight * weight * weight
            for dz in range(3):
                zz = (z + (dz - 1 + nz)) % nz
                lhs = left[dz * own + n]
                near = [(dx * sy + y + dy) * nz + zz for dx in range(3) for dy in range(3)]
                if dz == 1:
                    near.pop(4)
                while near:
                    pair, near = near[:2], near[2:]
                    rhs = [right[index] for index in pair]
                    rhs = jnp.concatenate(rhs, axis=1) if len(rhs) > 1 else rhs[0]
                    weight = jnp.maximum(dot(lhs, rhs, NN), 0.0)
                    cube = weight * weight * weight
                    for part in range(len(pair)):
                        total_sum = total_sum + cube[:, part * slots : (part + 1) * slots]
            column = jnp.sum(total_sum, axis=1, keepdims=True)
            sums[...] = jnp.where(lane == n, column, sums[...])
            return carry

        lax.fori_loop(0, own, one_cell, 0, unroll=4)
        rows = sums[...].T
        for y in range(cells_y):
            kind = channel(mid, y + 1, nz, 3)
            value = jnp.where(kind >= 0.0, rows[y * nz : (y + 1) * nz], 0.0)
            density[y] = value
            slope[pl.ds(y * nz, nz), :] = -by_kind(kind, embed) / (2.0 * jnp.sqrt(1.0 + value))

    return pl.pallas_call(
        kernel,
        out_shape=(
            pltpu.VMEM((cells_y, nz, slots), F32),
            pltpu.VMEM((own, slots), F32),
        ),
        in_specs=[VMEM, VMEM, VMEM, SMEM, SMEM],
        out_specs=(VMEM, VMEM),
        scratch_shapes=[
            pltpu.VMEM((total * 8, slots), F32),
            pltpu.VMEM((3 * own * 8, slots), F32),
            pltpu.VMEM((total, 48, slots), BF16),
            pltpu.VMEM((3 * own, slots, 48), BF16),
            pltpu.VMEM((slots, 128), F32),
        ],
        compiler_params=PARAMS,
        cost_estimate=pl.CostEstimate(
            flops=own * 27 * slots * slots * 40, bytes_accessed=total * slots * 16, transcendentals=0
        ),
        name="density",
    )


def make_force(cells_y, nz, slots):
    sy = cells_y + 2
    own = cells_y * nz
    total = 3 * sy * nz
    chunk = 64

    def kernel(
        low, mid, high, slope_low, slope_mid, slope_high, electrons, repel, out,
        feature, extra, own_feature, own_extra, place, right, right_extra, left, left_extra,
        sums,
    ):
        for ref in (feature, extra, own_feature, own_extra):
            ref[...] = jnp.zeros(ref.shape, F32)
        blocks = zip((low, mid, high), (slope_low, slope_mid, slope_high))
        for x, (block, slopes) in enumerate(blocks):
            for y in range(sy):
                pos = row_positions(block, x, y, sy, nz)
                square = pos[0] * pos[0] + pos[1] * pos[1] + pos[2] * pos[2]
                kind = channel(block, y, nz, 3)
                scale = by_kind(kind, repel)
                inverse = 1.0 / by_kind(kind, repel, 1.0)
                inverse = inverse * inverse
                steep = slopes[pl.ds(y * nz, nz), :] * inverse
                mild = -3.0 * by_kind(kind, electrons) * inverse
                base = (x * sy + y) * nz * 8
                feature[pl.ds(base, nz, stride=8), :] = scale * (1.0 - square)
                for d in range(3):
                    feature[pl.ds(base + 1 + d, nz, stride=8), :] = 2.0 * scale * pos[d]
                    place[pl.ds(base + d, nz, stride=8), :] = pos[d]
                feature[pl.ds(base + 4, nz, stride=8), :] = -scale
                extra[pl.ds(base, nz, stride=8), :] = steep
                extra[pl.ds(base + 1, nz, stride=8), :] = mild
                if x == 1 and 1 <= y <= cells_y:
                    base = (y - 1) * nz * 8
                    own_extra[pl.ds(base, nz, stride=8), :] = mild
                    own_extra[pl.ds(base + 1, nz, stride=8), :] = steep
                    for dz in range(3):
                        across = pos[2] - (dz - 1.0)
                        square = pos[0] * pos[0] + pos[1] * pos[1] + across * across
                        base = (dz * own + (y - 1) * nz) * 8
                        rows = (1.0, pos[0], pos[1], across, square)
                        for k, value in enumerate(rows):
                            own_feature[pl.ds(base + k, nz, stride=8), :] = scale * value

        def fill_right(n, carry):
            rows = pl.ds(n * 8, 8)
            right[n] = piece_rows(feature[rows, :], WIDE, 0).astype(BF16)
            right_extra[n] = piece_rows(extra[rows, :], SHORT, 0).astype(BF16)
            return carry

        def fill_left(n, carry):
            left[n] = piece_rows(own_feature[pl.ds(n * 8, 8), :], WIDE, 1).T.astype(BF16)
            return carry

        def fill_left_extra(n, carry):
            left_extra[n] = piece_rows(own_extra[pl.ds(n * 8, 8), :], SHORT, 1).T.astype(BF16)
            return carry

        lax.fori_loop(0, total, fill_right, 0, unroll=8)
        lax.fori_loop(0, 3 * own, fill_left, 0, unroll=8)
        lax.fori_loop(0, own, fill_left_extra, 0, unroll=8)
        same = same_slot(slots)
        lane = lax.broadcasted_iota(jnp.int32, (slots, 128), 1)
        sums[...] = jnp.zeros(sums.shape, F32)

        def one_cell(n, carry):
            y, z = n // nz, n % nz
            for start in range(0, slots, chunk):
                rows = pl.ds(start, chunk)
                lhs_extra = left_extra[n, rows, :]
                parts = [jnp.zeros((chunk, slots), F32) for _ in range(4)]
                for dz in range(3):
                    zz = (z + (dz - 1 + nz)) % nz
                    lhs = left[dz * own + n, rows, :]
                    near = [(dx * sy + y + dy) * nz + zz for dx in range(3) for dy in range(3)]
                    if dz == 1:
                        near.append(near.pop(4))
                    for index in range(0, 9, 2):
                        pair = near[index : index + 2]
                        rhs = [right[cell] for cell in pair]
                        rhs_extra = [right_extra[cell] for cell in pair]
                        if len(pair) > 1:
                            rhs = [jnp.concatenate(rhs, axis=1)]
                            rhs_extra = [jnp.concatenate(rhs_extra, axis=1)]
                        weight = jnp.maximum(dot(lhs, rhs[0], NN), 0.0)
                        if dz == 1 and index == 8:
                            weight = jnp.where(same[start : start + chunk], 0.0, weight)
                        value = (weight * dot(lhs_extra, rhs_extra[0], NN) - 2.0) * weight
                        for k, cell in enumerate(pair):
                            tile = value[:, k * slots : (k + 1) * slots]
                            parts[3] = parts[3] + tile
                            for d in range(3):
                                there = place[pl.ds(cell * 8 + d, 1), :]
                                if d == 2 and dz != 1:
                                    there = there + (dz - 1.0)
                                parts[d] = parts[d] + tile * there
                for d in range(4):
                    column = jnp.sum(parts[d], axis=1, keepdims=True)
                    sums[d, rows, :] = jnp.where(
                        lane[start : start + chunk] == n, column, sums[d, rows, :]
                    )
            return carry

        lax.fori_loop(0, own, one_cell, 0, unroll=4)
        rows = [sums[d].T for d in range(4)]
        for y in range(cells_y):
            pos = row_positions(mid, 1, y + 1, sy, nz)
            part = slice(y * nz, (y + 1) * nz)
            for d in range(3):
                out[d, y] = 2.0 * (rows[d][part] - pos[d] * rows[3][part])

    return pl.pallas_call(
        kernel,
        out_shape=pltpu.VMEM((3, cells_y, nz, slots), F32),
        in_specs=[VMEM] * 6 + [SMEM, SMEM],
        out_specs=VMEM,
        scratch_shapes=[
            pltpu.VMEM((total * 8, slots), F32),
            pltpu.VMEM((total * 8, slots), F32),
            pltpu.VMEM((3 * own * 8, slots), F32),
            pltpu.VMEM((own * 8, slots), F32),
            pltpu.VMEM((total * 8, slots), F32),
            pltpu.VMEM((total, 48, slots), BF16),
            pltpu.VMEM((total, 32, slots), BF16),
            pltpu.VMEM((3 * own, slots, 48), BF16),
            pltpu.VMEM((own, slots, 32), BF16),
            pltpu.VMEM((4, slots, 128), F32),
        ],
        compiler_params=PARAMS,
        cost_estimate=pl.CostEstimate(
            flops=own * 27 * slots * slots * 100,
            bytes_accessed=total * slots * 16,
            transcendentals=0,
        ),
        name="force",
    )


def shifted(axis, count):
    up = [(i, (i + 1) % count) for i in range(count)]
    down = [(target, source) for source, target in up]
    return lambda part: lax.ppermute(part, axis, up), lambda part: lax.ppermute(part, axis, down)


def halo(block, rows, gx, gy, gz):
    up, down = shifted("gy", gy)
    if gy == 2 and block.shape[0] == 2 * rows:
        other = up(block)
        low, high = other[-rows:], other[:rows]
    else:
        low, high = up(block[-rows:]), down(block[:rows])
    middle = jnp.concatenate([low, block, high], axis=0)
    up, down = shifted(("gx", "gz"), gx * gz)
    low = up(middle)
    high = down(middle)
    return low, middle, high


def on_device(
    cell_counts,
    grid_offset,
    fraction,
    species,
    species_density,
    species_pair,
    species_embed,
    species_charge,
):
    cells_x, cells_y, cells_z, _, slots = fraction.shape
    gx, gy, gz = (lax.axis_size(name) for name in ("gx", "gy", "gz"))
    devices = gx * gy * gz
    assert cells_x == gz and slots == 128
    lx, ly, lz = cells_x * gx * PPC, cells_y * gy * PPC, cells_z * gz * PPC
    assert lz % devices == 0
    modes = lz // devices
    yl = cells_y * PPC
    relayout = modes <= 128 and yl % max(1, 128 // modes) == 0

    slot_index = lax.broadcasted_iota(jnp.int32, species.shape, 3)
    alive = slot_index < cell_counts[..., None]
    kind = jnp.where(alive, species.astype(F32), -1.0)[:, :, None]

    atoms = jnp.concatenate(
        [
            grid_offset.astype(F32).transpose(0, 1, 3, 2, 4),
            fraction.transpose(0, 1, 3, 2, 4),
            kind,
        ],
        axis=2,
    )
    atoms = lax.all_to_all(atoms, "gz", split_axis=0, concat_axis=0, tiled=True)
    basis_x, basis_z = real_basis(lx), real_basis(lz)
    x_pair, xt_pair, z_pair = table_pair(basis_x), table_pair(basis_x.T), table_pair(basis_z)
    y_pair = table_pair(np.kron(real_basis(ly), np.eye(modes)))
    spread = make_spread(gz, cells_y, cells_z, slots, lz, devices, relayout)
    lines = spread(near_core(atoms), species_charge, z_pair)
    if not relayout:
        lines = lines.reshape(yl, PPC, devices, modes).transpose(2, 1, 0, 3)
        lines = lines.reshape(devices, PPC, yl * modes)
    planes = lax.all_to_all(lines, ("gx", "gy", "gz"), split_axis=0, concat_axis=0, tiled=True)

    nz = gz * cells_z
    place = (atoms[:, :, 0:3] + 0.5 + atoms[:, :, 3:6]) / PPC - 0.5
    place = jnp.concatenate([place, atoms[:, :, 6:7]], axis=2)
    place = place.transpose(1, 2, 0, 3, 4).reshape(cells_y * 4 * nz, slots)
    near = halo(place, nz * 4, gx, gy, gz)
    density, slope = make_density(cells_y, nz, slots)(
        *map(near_core, near), species_density, species_embed
    )
    near_slopes = halo(slope, nz, gx, gy, gz)

    rank = lax.axis_index(("gx", "gy", "gz")).astype(jnp.int32).reshape(1)
    planes = make_planes(gx, gy, gz, yl * modes, lx, ly, lz)(
        rank, near_core(planes), x_pair, xt_pair, y_pair
    )
    lines = lax.all_to_all(planes, ("gx", "gy", "gz"), split_axis=0, concat_axis=0, tiled=True)
    if not relayout:
        lines = lines.reshape(devices, PPC, yl, modes).transpose(2, 1, 0, 3)
        lines = lines.reshape(yl * PPC, lz)

    short = make_force(cells_y, nz, slots)(
        *map(near_core, near), *map(near_core, near_slopes), species_density, species_pair
    )
    result = make_sample(gz, cells_y, cells_z, slots, lz, devices, relayout)(
        near_core(lines), near_core(atoms), near_core(short), near_core(density), species_charge, z_pair
    )
    result = lax.all_to_all(result, "gz", split_axis=0, concat_axis=0, tiled=True)
    return (result[:, :, 0:3].transpose(0, 1, 3, 2, 4), result[:, :, 3])


def solution(mesh):
    return jax.shard_map(
        on_device,
        mesh=mesh,
        in_specs=(
            P("gx", "gy", "gz"),
            P("gx", "gy", "gz", None, None),
            P("gx", "gy", "gz", None, None),
            P("gx", "gy", "gz", None),
            P(),
            P(),
            P(),
            P(),
        ),
        out_specs=(P("gx", "gy", "gz", None, None), P("gx", "gy", "gz", None)),
        check_vma=False,
    )
```

```python
import math

import ml_dtypes
import numpy as np

import jax
import jax.numpy as jnp
from jax import lax
from jax.experimental import pallas as pl
from jax.experimental.pallas import tpu as pltpu
from jax.sharding import PartitionSpec as P


NSPEC = 2
PPC = 16
EWALD_SPLIT = 0.7
COUPLING = 8.0
F32 = jnp.float32
BF16 = jnp.bfloat16
VMEM = pl.BlockSpec(memory_space=pltpu.VMEM)
SMEM = pl.BlockSpec(memory_space=pltpu.SMEM)
ANY = pl.BlockSpec(memory_space=pl.ANY)
NN = (((1,), (0,)), ((), ()))
NT = (((1,), (1,)), ((), ()))
PARAMS = pltpu.CompilerParams(vmem_limit_bytes=56 * 1024 * 1024)


def near_core(values):
    return pltpu.with_memory_space_constraint(values, pltpu.VMEM)


def split2(values):
    high = values.astype(BF16)
    return high, (values - high.astype(F32)).astype(BF16)


def split3(values):
    high = values.astype(BF16).astype(F32)
    rest = values - high
    middle = rest.astype(BF16).astype(F32)
    return high, middle, (rest - middle).astype(BF16).astype(F32)


def dot(left, right, dims):
    return lax.dot_general(left, right, dims, preferred_element_type=F32)


def stack2(values):
    high, low = split2(values)
    return jnp.concatenate([high, low], axis=0)


def dot3(left, right, dims):
    rows = left.shape[0] // 2
    wide = dot(left, right[0], dims)
    return wide[:rows] + wide[rows:] + dot(left[:rows], right[1], dims)


def by_kind(kind, table, empty=0.0):
    result = jnp.full(kind.shape, empty, F32)
    for kind_index in range(NSPEC):
        result = jnp.where(kind == float(kind_index), table[kind_index], result)
    return result


def real_basis(length):
    rows = np.arange(length)[:, None]
    points = np.arange(length)[None, :]
    half = length // 2
    waves = np.where(rows <= half, rows, length - rows)
    angle = 2.0 * np.pi * ((waves * points) % length) / length
    basis = np.where(rows <= half, np.cos(angle), np.sin(angle)) * math.sqrt(2.0 / length)
    basis[0] *= math.sqrt(0.5)
    basis[half] *= math.sqrt(0.5)
    return basis


def table_pair(values):
    values = values.astype(np.float32)
    high = values.astype(ml_dtypes.bfloat16)
    low = (values - high.astype(np.float32)).astype(ml_dtypes.bfloat16)
    return jnp.asarray(np.stack([high, low]))


def signed_modes(indices, total):
    return jnp.where(2 * indices >= total, indices - total, indices)


def chunk_transpose(tiles, chunk):
    tiles = list(tiles)
    count = len(tiles)
    width = tiles[0].shape[-1]
    lane_chunk = lax.broadcasted_iota(jnp.int32, tiles[0].shape, 1) // chunk
    bit = 1
    while bit < count:
        keep = (lane_chunk & bit) == 0
        for low in range(count):
            if low & bit:
                continue
            first, second = tiles[low], tiles[low | bit]
            tiles[low] = jnp.where(keep, first, pltpu.roll(second, bit * chunk, 1))
            tiles[low | bit] = jnp.where(keep, pltpu.roll(first, width - bit * chunk, 1), second)
        bit *= 2
    return tiles


def point_weights(offset_row, fraction_row):
    points = lax.broadcasted_iota(jnp.int32, (PPC, offset_row.shape[-1]), 0).astype(F32)
    lower = points == offset_row
    upper = points == offset_row + 1.0
    weights = jnp.where(lower, 1.0 - fraction_row, jnp.where(upper, fraction_row, 0.0))
    slopes = jnp.where(lower, -1.0, jnp.where(upper, 1.0, 0.0))
    return weights, slopes


def make_spread(parts, cells_y, cells_z, slots, lz, devices, relayout):
    columns = parts * cells_z
    modes = lz // devices
    yl = cells_y * PPC
    rows = PPC * PPC

    tiles = lz // 128
    reach = columns // tiles

    def kernel(atoms, table, basis_any, out, plane, line, basis_ref, sem):
        fetch = pltpu.make_async_copy(basis_any, basis_ref, sem)
        fetch.start()
        line[...] = jnp.zeros(line.shape, BF16)
        pieces = []
        for cy in range(cells_y):
            brick = []
            for tile in range(tiles):
                for place in range(reach):
                    column = tile * reach + place
                    cell = atoms[column // cells_z, cy, :, column % cells_z, :]
                    weights = [
                        point_weights(cell[d : d + 1], cell[3 + d : 4 + d])[0] for d in range(3)
                    ]
                    along_x = weights[0] * by_kind(cell[6:7], table)
                    value = jnp.concatenate(
                        [weights[1][y : y + 1] * along_x for y in range(PPC)], axis=0
                    )
                    lanes = pl.ds(place * slots, slots)
                    high, low = split2(value)
                    plane[tile, pl.ds(0, rows), lanes] = high
                    plane[tile, pl.ds(rows, rows), lanes] = low
                    high, low = split2(weights[2])
                    line[tile, pl.ds(place * PPC, PPC), lanes] = high
                    line[tile, pl.ds(128 + place * PPC, PPC), lanes] = low
                wide = dot(plane[tile], line[tile], NT)
                wide = wide[:rows] + wide[rows:]
                brick.append(wide[:, :128] + wide[:, 128:])
            if cy == 0:
                fetch.wait()
            brick = jnp.concatenate(brick, axis=1)
            pieces.append(dot3(stack2(brick), (basis_ref[0], basis_ref[1]), NT))
        if not relayout:
            for cy in range(cells_y):
                out[pl.ds(cy * rows, rows), :] = pieces[cy]
            return
        chunks = 128 // modes
        for tile in range(tiles):
            for group in range(yl // chunks):
                parts = []
                for y in range(group * chunks, (group + 1) * chunks):
                    start = (y % PPC) * PPC
                    parts.append(
                        pieces[y // PPC][start : start + PPC, tile * 128 : tile * 128 + 128]
                    )
                for chunk, value in enumerate(chunk_transpose(parts, modes)):
                    out[tile * chunks + chunk, :, pl.ds(group * 128, 128)] = value

    if relayout:
        shape = (devices, PPC, yl * modes)
    else:
        shape = (cells_y * rows, lz)
    return pl.pallas_call(
        kernel,
        out_shape=pltpu.VMEM(shape, F32),
        in_specs=[VMEM, SMEM, ANY],
        out_specs=VMEM,
        scratch_shapes=[
            pltpu.VMEM((tiles, 2 * rows, reach * slots), BF16),
            pltpu.VMEM((tiles, 256, reach * slots), BF16),
            pltpu.VMEM((2, lz, lz), BF16),
            pltpu.SemaphoreType.DMA(()),
        ],
        compiler_params=PARAMS,
        name="spread",
    )


def make_planes(gx, gy, gz, lanes, lx, ly, lz):
    modes = lz // (gx * gy * gz)
    width = ly * modes
    sharp = -1.0 / (4.0 * EWALD_SPLIT * EWALD_SPLIT)

    def wave_square(indices, length):
        return jnp.square(signed_modes(indices, length).astype(F32) * (2.0 * math.pi / length))

    def kernel(rank, data, x_any, xt_any, y_any, out, grid, x_ref, xt_ref, y_ref, sems):
        fetches = [
            pltpu.make_async_copy(source, target, sems.at[index])
            for index, (source, target) in enumerate(
                ((x_any, x_ref), (y_any, y_ref), (xt_any, xt_ref))
            )
        ]
        for fetch in fetches:
            fetch.start()
        for a in range(gx):
            for b in range(gy):
                for c in range(gz):
                    grid[pl.ds((a * gz + c) * PPC, PPC), pl.ds(b * lanes, lanes)] = data[
                        (a * gy + b) * gz + c
                    ]
        lane = lax.broadcasted_iota(jnp.int32, (1, width), 1)
        across = wave_square(lane // modes, ly) + wave_square(rank[0] * modes + lane % modes, lz)
        along = wave_square(lax.broadcasted_iota(jnp.int32, (lx, 1), 0), lx)
        squared = along + across
        factor = (4.0 * math.pi * jnp.exp(along * sharp)) * jnp.exp(across * sharp)
        green = jnp.where(squared == 0.0, 0.0, factor / jnp.where(squared == 0.0, 1.0, squared))
        fetches[0].wait()
        value = dot3(x_ref[...], split2(grid[...]), NN)
        fetches[1].wait()
        value = dot3(stack2(value), (y_ref[0], y_ref[1]), NT) * green
        value = dot3(stack2(value), (y_ref[0], y_ref[1]), NN)
        fetches[2].wait()
        value = dot3(xt_ref[...], split2(value), NN)
        for a in range(gx):
            for b in range(gy):
                for c in range(gz):
                    start = (a * gz + c) * PPC
                    out[(a * gy + b) * gz + c] = value[
                        start : start + PPC, b * lanes : (b + 1) * lanes
                    ]

    return pl.pallas_call(
        kernel,
        out_shape=pltpu.VMEM((gx * gy * gz, PPC, lanes), F32),
        in_specs=[SMEM, VMEM, ANY, ANY, ANY],
        out_specs=VMEM,
        scratch_shapes=[
            pltpu.VMEM((lx, width), F32),
            pltpu.VMEM((2 * lx, lx), BF16),
            pltpu.VMEM((2 * lx, lx), BF16),
            pltpu.VMEM((2, width, width), BF16),
            pltpu.SemaphoreType.DMA((3,)),
        ],
        compiler_params=PARAMS,
        name="planes",
    )


def make_sample(parts, cells_y, cells_z, slots, lz, devices, relayout):
    columns = parts * cells_z
    modes = lz // devices
    yl = cells_y * PPC
    rows = PPC * PPC

    reach = columns * 128 // lz

    def kernel(
        data, atoms, short, dens, table, basis_any, out, lines, line, basis_ref, sem
    ):
        fetch = pltpu.make_async_copy(basis_any, basis_ref, sem)
        fetch.start()
        if relayout:
            chunks = 128 // modes
            for tile in range(lz // 128):
                for group in range(yl // chunks):
                    tiles = [
                        data[tile * chunks + chunk, :, pl.ds(group * 128, 128)]
                        for chunk in range(chunks)
                    ]
                    for index, value in enumerate(chunk_transpose(tiles, modes)):
                        lines[
                            pl.ds((group * chunks + index) * PPC, PPC), pl.ds(tile * 128, 128)
                        ] = value
        else:
            lines[...] = data[...]
        line[...] = jnp.zeros(line.shape, BF16)
        fetch.wait()
        for cy in range(cells_y):
            brick = dot3(
                stack2(lines[pl.ds(cy * rows, rows), :]), (basis_ref[0], basis_ref[1]), NN
            )
            for column in range(columns):
                if column % reach == 0:
                    start = column // reach * 128
                    value = brick[:, start : start + 128]
                    high = value.astype(BF16)
                    left_half = lax.broadcasted_iota(jnp.int32, value.shape, 1) < 64
                    top = high.astype(F32)
                    swapped = pltpu.roll(value - top, 64, 1)
                    wides = [
                        jnp.concatenate([half.astype(BF16), high], axis=1)
                        for half in (
                            jnp.where(left_half, top, swapped),
                            jnp.where(left_half, swapped, top),
                        )
                    ]
                wide = wides[column % reach * 2 // reach]
                cell = atoms[column // cells_z, cy, :, column % cells_z, :]
                pairs = [point_weights(cell[d : d + 1], cell[3 + d : 4 + d]) for d in range(3)]
                (wx, sx), (wy, sy), (wz, sz) = pairs
                first = column % reach * PPC
                high, low = split2(wz)
                both = jnp.concatenate([high, sz.astype(BF16)], axis=1)
                line[column, pl.ds(first, PPC), :] = both
                line[column, pl.ds((first + 64) % 128, PPC), :] = both
                line[column, pl.ds(128 + first, PPC), pl.ds(0, slots)] = low
                both = dot(wide, line[column], NN)
                plain, tilted = both[:, :slots], both[:, slots:]
                force_x = jnp.zeros((PPC, slots), F32)
                force_y = jnp.zeros((PPC, slots), F32)
                force_z = jnp.zeros((PPC, slots), F32)
                for y in range(PPC):
                    block = plain[y * PPC : (y + 1) * PPC]
                    force_x += wy[y : y + 1] * block
                    force_y += sy[y : y + 1] * block
                    force_z += wy[y : y + 1] * tilted[y * PPC : (y + 1) * PPC]
                charge = -COUPLING * by_kind(cell[6:7], table)
                here = pl.ds(column, 1)
                result = [
                    charge * jnp.sum(force * weight, axis=0, keepdims=True)
                    + short[d, cy, here, :]
                    for d, (force, weight) in enumerate(
                        ((force_x, sx), (force_y, wx), (force_z, wx))
                    )
                ]
                result = [jnp.where(cell[6:7] >= 0.0, value, 0.0) for value in result]
                result.append(dens[cy, here, :])
                out[column // cells_z, cy, :, column % cells_z, :] = jnp.concatenate(result, axis=0)

    return pl.pallas_call(
        kernel,
        out_shape=pltpu.VMEM((parts, cells_y, 4, cells_z, slots), F32),
        in_specs=[VMEM, VMEM, VMEM, VMEM, SMEM, ANY],
        out_specs=VMEM,
        scratch_shapes=[
            pltpu.VMEM((cells_y * rows, lz), F32),
            pltpu.VMEM((columns, 256, 2 * slots), BF16),
            pltpu.VMEM((2, lz, lz), BF16),
            pltpu.SemaphoreType.DMA(()),
        ],
        compiler_params=PARAMS,
        name="sample",
    )


RIGHT = ((0, 0), (1, 0), (1, 0), (2, 0))
LEFT = ((0, 1), (0, 1), (1, 2), (0, 2))


def clear_spare(ref):
    count = ref.shape[1] // 8
    for tile in (1, 3):
        ref[tile, pl.ds(7, count, stride=8), :] = jnp.zeros((count, ref.shape[2]), F32)


def store_five(ref, first, count, values, order):
    pieces = [split3(value) for value in values]
    for tile, (main, third) in enumerate(order):
        rows = [pieces[index][main] for index in range(5)]
        rows += [pieces[index][third] for index in ((3, 4) if tile % 2 else (0, 1, 2))]
        for row, value in enumerate(rows):
            ref[tile, pl.ds(first * 8 + row, count, stride=8), :] = value


def five_rows(ref, cell):
    tiles = [ref[tile, pl.ds(cell * 8, 8), :] for tile in range(4)]
    return jnp.concatenate(tiles, axis=0).astype(BF16)


def fill(feature, own_feature, right, left):
    def fill_right(n, carry):
        right[n] = five_rows(feature, n)
        return carry

    def fill_left(n, carry):
        left[n] = five_rows(own_feature, n).T
        return carry

    lax.fori_loop(0, right.shape[0], fill_right, 0, unroll=8)
    lax.fori_loop(0, left.shape[0], fill_left, 0, unroll=8)


def two_rows(values, side):
    high = values.astype(BF16).astype(F32)
    rest = values - high
    row = lax.broadcasted_iota(jnp.int32, values.shape, 0)
    pick = row < 4 if side else row % 4 < 2
    return jnp.concatenate([jnp.where(pick, high, rest), jnp.zeros_like(values)], axis=0)


def channel(block, y, nz, index):
    return block[pl.ds((y * 4 + index) * nz, nz), :]


def row_positions(block, x, y, sy, nz):
    pos_x = channel(block, y, nz, 0) + (x - 1.0)
    pos_y = channel(block, y, nz, 1) + (y - 0.5 * (sy - 1))
    return pos_x, pos_y, channel(block, y, nz, 2)


def same_slot(slots):
    return lax.broadcasted_iota(jnp.int32, (slots, slots), 0) == lax.broadcasted_iota(
        jnp.int32, (slots, slots), 1
    )


def make_density(cells_y, nz, slots):
    sy = cells_y + 2
    own = cells_y * nz
    total = 3 * sy * nz

    def kernel(
        low, mid, high, electrons, embed, density, slope, feature, own_feature, right, left, sums
    ):
        clear_spare(feature)
        clear_spare(own_feature)
        for x, block in enumerate((low, mid, high)):
            for y in range(sy):
                pos = row_positions(block, x, y, sy, nz)
                square = pos[0] * pos[0] + pos[1] * pos[1] + pos[2] * pos[2]
                kind = channel(block, y, nz, 3)
                scale = jnp.exp(jnp.log(by_kind(kind, electrons, 1.0)) * (1.0 / 3.0))
                scale = jnp.where(kind >= 0.0, scale, 0.0)
                double = 2.0 * scale
                values = [scale * (1.0 - square)] + [double * pos[d] for d in range(3)] + [-scale]
                store_five(feature, (x * sy + y) * nz, nz, values, RIGHT)
                if x == 1 and 1 <= y <= cells_y:
                    for dz in range(3):
                        across = pos[2] - (dz - 1.0)
                        square = pos[0] * pos[0] + pos[1] * pos[1] + across * across
                        values = [jnp.ones_like(square), pos[0], pos[1], across, square]
                        store_five(own_feature, dz * own + (y - 1) * nz, nz, values, LEFT)

        fill(feature, own_feature, right, left)
        same = same_slot(slots)
        lane = lax.broadcasted_iota(jnp.int32, (slots, 128), 1)
        sums[...] = jnp.zeros(sums.shape, F32)

        def one_cell(n, carry):
            y, z = n // nz, n % nz
            weight = jnp.maximum(dot(left[own + n], right[(sy + y + 1) * nz + z], NN), 0.0)
            weight = jnp.where(same, 0.0, weight)
            total_sum = weight * weight * weight
            for dz in range(3):
                zz = (z + (dz - 1 + nz)) % nz
                lhs = left[dz * own + n]
                near = [(dx * sy + y + dy) * nz + zz for dx in range(3) for dy in range(3)]
                if dz == 1:
                    near.pop(4)
                while near:
                    pair, near = near[:2], near[2:]
                    rhs = [right[index] for index in pair]
                    rhs = jnp.concatenate(rhs, axis=1) if len(rhs) > 1 else rhs[0]
                    weight = jnp.maximum(dot(lhs, rhs, NN), 0.0)
                    cube = weight * weight * weight
                    for part in range(len(pair)):
                        total_sum = total_sum + cube[:, part * slots : (part + 1) * slots]
            column = jnp.sum(total_sum, axis=1, keepdims=True)
            sums[...] = jnp.where(lane == n, column, sums[...])
            return carry

        lax.fori_loop(0, own, one_cell, 0, unroll=4)
        rows = sums[...].T
        for y in range(cells_y):
            kind = channel(mid, y + 1, nz, 3)
            value = jnp.where(kind >= 0.0, rows[y * nz : (y + 1) * nz], 0.0)
            density[y] = value
            slope[pl.ds(y * nz, nz), :] = -by_kind(kind, embed) / (2.0 * jnp.sqrt(1.0 + value))

    return pl.pallas_call(
        kernel,
        out_shape=(
            pltpu.VMEM((cells_y, nz, slots), F32),
            pltpu.VMEM((own, slots), F32),
        ),
        in_specs=[VMEM, VMEM, VMEM, SMEM, SMEM],
        out_specs=(VMEM, VMEM),
        scratch_shapes=[
            pltpu.VMEM((4, total * 8, slots), F32),
            pltpu.VMEM((4, 3 * own * 8, slots), F32),
            pltpu.VMEM((total, 32, slots), BF16),
            pltpu.VMEM((3 * own, slots, 32), BF16),
            pltpu.VMEM((slots, 128), F32),
        ],
        compiler_params=PARAMS,
        cost_estimate=pl.CostEstimate(
            flops=own * 27 * slots * slots * 40, bytes_accessed=total * slots * 16, transcendentals=0
        ),
        name="density",
    )


def make_force(cells_y, nz, slots):
    sy = cells_y + 2
    own = cells_y * nz
    total = 3 * sy * nz
    chunk = 8

    def kernel(
        low, mid, high, slope_low, slope_mid, slope_high, electrons, repel, out,
        feature, extra, own_feature, own_extra, place, right, right_extra, left, left_extra, acc, sums,
    ):
        clear_spare(feature)
        clear_spare(own_feature)
        blocks = zip((low, mid, high), (slope_low, slope_mid, slope_high))
        for x, (block, slopes) in enumerate(blocks):
            for y in range(sy):
                pos = row_positions(block, x, y, sy, nz)
                square = pos[0] * pos[0] + pos[1] * pos[1] + pos[2] * pos[2]
                kind = channel(block, y, nz, 3)
                scale = by_kind(kind, repel)
                inverse = 1.0 / by_kind(kind, repel, 1.0)
                inverse = inverse * inverse
                steep = slopes[pl.ds(y * nz, nz), :] * inverse
                mild = -3.0 * by_kind(kind, electrons) * inverse
                double = 2.0 * scale
                values = [scale * (1.0 - square)] + [double * pos[d] for d in range(3)] + [-scale]
                cell = (x * sy + y) * nz
                store_five(feature, cell, nz, values, RIGHT)
                for d in range(3):
                    place[pl.ds(cell * 8 + d, nz, stride=8), :] = pos[d]
                for k in range(8):
                    extra[pl.ds(cell * 8 + k, nz, stride=8), :] = mild if k % 2 else steep
                if x == 1 and 1 <= y <= cells_y:
                    cell = (y - 1) * nz
                    for k in range(8):
                        own_extra[pl.ds(cell * 8 + k, nz, stride=8), :] = steep if k % 2 else mild
                    for dz in range(3):
                        across = pos[2] - (dz - 1.0)
                        square = pos[0] * pos[0] + pos[1] * pos[1] + across * across
                        values = [scale] + [
                            scale * value for value in (pos[0], pos[1], across, square)
                        ]
                        store_five(own_feature, dz * own + cell, nz, values, LEFT)

        fill(feature, own_feature, right, left)

        def fill_right_extra(n, carry):
            right_extra[n] = two_rows(extra[pl.ds(n * 8, 8), :], 0).astype(BF16)
            return carry

        def fill_left_extra(n, carry):
            left_extra[n] = two_rows(own_extra[pl.ds(n * 8, 8), :], 1).astype(BF16).T
            return carry

        lax.fori_loop(0, total, fill_right_extra, 0, unroll=8)
        lax.fori_loop(0, own, fill_left_extra, 0, unroll=8)
        same = same_slot(slots)
        lane = lax.broadcasted_iota(jnp.int32, (slots, 128), 1)
        sums[...] = jnp.zeros(sums.shape, F32)

        def one_cell(n, carry):
            y, z = n // nz, n % nz
            lhs_extra = left_extra[n]
            first = True
            for dz in range(3):
                zz = (z + (dz - 1 + nz)) % nz
                lhs = left[dz * own + n]
                near = [(dx * sy + y + dy) * nz + zz for dx in range(3) for dy in range(3)]
                if dz == 1:
                    near.append(near.pop(4))
                for index in range(0, 9, 2):
                    pair = near[index : index + 2]
                    rhs = [right[cell] for cell in pair]
                    rhs_extra = [right_extra[cell] for cell in pair]
                    if len(pair) > 1:
                        rhs = [jnp.concatenate(rhs, axis=1)]
                        rhs_extra = [jnp.concatenate(rhs_extra, axis=1)]
                    weight = jnp.maximum(dot(lhs, rhs[0], NN), 0.0)
                    if dz == 1 and index == 8:
                        weight = jnp.where(same, 0.0, weight)
                    value = (weight * dot(lhs_extra, rhs_extra[0], NN) - 2.0) * weight
                    there = [
                        [place[pl.ds(cell * 8 + d, 1), :] for d in range(3)] for cell in pair
                    ]
                    if dz != 1:
                        there = [[x, y_, z_ + (dz - 1.0)] for x, y_, z_ in there]
                    for start in range(0, slots, chunk):
                        rows = pl.ds(start, chunk)
                        tiles = [
                            value[start : start + chunk, k * slots : (k + 1) * slots]
                            for k in range(len(pair))
                        ]
                        sums_of = [
                            [tile * there[k][d] for k, tile in enumerate(tiles)] for d in range(3)
                        ] + [tiles]
                        for d in range(4):
                            part = sums_of[d][0]
                            for more in sums_of[d][1:]:
                                part = part + more
                            acc[d, rows, :] = part if first else acc[d, rows, :] + part
                    first = False
            for d in range(4):
                column = jnp.sum(acc[d], axis=1, keepdims=True)
                sums[d] = jnp.where(lane == n, column, sums[d])
            return carry

        lax.fori_loop(0, own, one_cell, 0, unroll=4)
        rows = [sums[d].T for d in range(4)]
        for y in range(cells_y):
            pos = row_positions(mid, 1, y + 1, sy, nz)
            part = slice(y * nz, (y + 1) * nz)
            for d in range(3):
                out[d, y] = 2.0 * (rows[d][part] - pos[d] * rows[3][part])

    return pl.pallas_call(
        kernel,
        out_shape=pltpu.VMEM((3, cells_y, nz, slots), F32),
        in_specs=[VMEM] * 6 + [SMEM, SMEM],
        out_specs=VMEM,
        scratch_shapes=[
            pltpu.VMEM((4, total * 8, slots), F32),
            pltpu.VMEM((total * 8, slots), F32),
            pltpu.VMEM((4, 3 * own * 8, slots), F32),
            pltpu.VMEM((own * 8, slots), F32),
            pltpu.VMEM((total * 8, slots), F32),
            pltpu.VMEM((total, 32, slots), BF16),
            pltpu.VMEM((total, 16, slots), BF16),
            pltpu.VMEM((3 * own, slots, 32), BF16),
            pltpu.VMEM((own, slots, 16), BF16),
            pltpu.VMEM((4, slots, slots), F32),
            pltpu.VMEM((4, slots, 128), F32),
        ],
        compiler_params=PARAMS,
        cost_estimate=pl.CostEstimate(
            flops=own * 27 * slots * slots * 100,
            bytes_accessed=total * slots * 16,
            transcendentals=0,
        ),
        name="force",
    )


def shifted(axis, count):
    up = [(i, (i + 1) % count) for i in range(count)]
    down = [(target, source) for source, target in up]
    return lambda part: lax.ppermute(part, axis, up), lambda part: lax.ppermute(part, axis, down)


def halo(block, rows, gx, gy, gz):
    up, down = shifted("gy", gy)
    if gy == 2 and block.shape[0] == 2 * rows:
        other = up(block)
        low, high = other[-rows:], other[:rows]
    else:
        low, high = up(block[-rows:]), down(block[:rows])
    middle = jnp.concatenate([low, block, high], axis=0)
    up, down = shifted(("gx", "gz"), gx * gz)
    low = up(middle)
    high = down(middle)
    return low, middle, high


def on_device(
    cell_counts,
    grid_offset,
    fraction,
    species,
    species_density,
    species_pair,
    species_embed,
    species_charge,
):
    cells_x, cells_y, cells_z, _, slots = fraction.shape
    gx, gy, gz = (lax.axis_size(name) for name in ("gx", "gy", "gz"))
    devices = gx * gy * gz
    assert cells_x == gz and slots == 128
    lx, ly, lz = cells_x * gx * PPC, cells_y * gy * PPC, cells_z * gz * PPC
    assert lz % devices == 0
    modes = lz // devices
    yl = cells_y * PPC
    relayout = modes <= 128 and yl % max(1, 128 // modes) == 0

    slot_index = lax.broadcasted_iota(jnp.int32, species.shape, 3)
    alive = slot_index < cell_counts[..., None]
    kind = jnp.where(alive, species.astype(F32), -1.0)[:, :, None]

    atoms = jnp.concatenate(
        [
            grid_offset.astype(F32).transpose(0, 1, 3, 2, 4),
            fraction.transpose(0, 1, 3, 2, 4),
            kind,
        ],
        axis=2,
    )
    atoms = lax.all_to_all(atoms, "gz", split_axis=0, concat_axis=0, tiled=True)
    basis_x, basis_z = real_basis(lx), real_basis(lz)
    x_pair, xt_pair, z_pair = table_pair(basis_x), table_pair(basis_x.T), table_pair(basis_z)
    y_pair = table_pair(np.kron(real_basis(ly), np.eye(modes)))
    spread = make_spread(gz, cells_y, cells_z, slots, lz, devices, relayout)
    lines = spread(near_core(atoms), species_charge, z_pair)
    if not relayout:
        lines = lines.reshape(yl, PPC, devices, modes).transpose(2, 1, 0, 3)
        lines = lines.reshape(devices, PPC, yl * modes)
    planes = lax.all_to_all(lines, ("gx", "gy", "gz"), split_axis=0, concat_axis=0, tiled=True)

    nz = gz * cells_z
    place = (atoms[:, :, 0:3] + 0.5 + atoms[:, :, 3:6]) / PPC - 0.5
    place = jnp.concatenate([place, atoms[:, :, 6:7]], axis=2)
    place = place.transpose(1, 2, 0, 3, 4).reshape(cells_y * 4 * nz, slots)
    near = halo(place, nz * 4, gx, gy, gz)
    density, slope = make_density(cells_y, nz, slots)(
        *map(near_core, near), species_density, species_embed
    )
    near_slopes = halo(slope, nz, gx, gy, gz)

    rank = lax.axis_index(("gx", "gy", "gz")).astype(jnp.int32).reshape(1)
    planes = make_planes(gx, gy, gz, yl * modes, lx, ly, lz)(
        rank, near_core(planes), x_pair.reshape(2 * lx, lx), xt_pair.reshape(2 * lx, lx), y_pair
    )
    lines = lax.all_to_all(planes, ("gx", "gy", "gz"), split_axis=0, concat_axis=0, tiled=True)
    if not relayout:
        lines = lines.reshape(devices, PPC, yl, modes).transpose(2, 1, 0, 3)
        lines = lines.reshape(yl * PPC, lz)

    operands = (*near, *near_slopes)
    short = make_force(cells_y, nz, slots)(*map(near_core, operands), species_density, species_pair)
    result = make_sample(gz, cells_y, cells_z, slots, lz, devices, relayout)(
        near_core(lines), near_core(atoms), near_core(short), near_core(density), species_charge, z_pair
    )
    result = lax.all_to_all(result, "gz", split_axis=0, concat_axis=0, tiled=True)
    return (result[:, :, 0:3].transpose(0, 1, 3, 2, 4), result[:, :, 3])


def solution(mesh):
    return jax.shard_map(
        on_device,
        mesh=mesh,
        in_specs=(
            P("gx", "gy", "gz"),
            P("gx", "gy", "gz", None, None),
            P("gx", "gy", "gz", None, None),
            P("gx", "gy", "gz", None),
            P(),
            P(),
            P(),
            P(),
        ),
        out_specs=(P("gx", "gy", "gz", None, None), P("gx", "gy", "gz", None)),
        check_vma=False,
    )
```

```python
import math

import ml_dtypes
import numpy as np

import jax
import jax.numpy as jnp
from jax import lax
from jax.experimental import pallas as pl
from jax.experimental.pallas import tpu as pltpu
from jax.sharding import PartitionSpec as P


NSPEC = 2
PPC = 16
EWALD_SPLIT = 0.7
COUPLING = 8.0
F32 = jnp.float32
BF16 = jnp.bfloat16
VMEM = pl.BlockSpec(memory_space=pltpu.VMEM)
SMEM = pl.BlockSpec(memory_space=pltpu.SMEM)
ANY = pl.BlockSpec(memory_space=pl.ANY)
NN = (((1,), (0,)), ((), ()))
NT = (((1,), (1,)), ((), ()))
PARAMS = pltpu.CompilerParams(vmem_limit_bytes=56 * 1024 * 1024)


def near_core(values):
    return pltpu.with_memory_space_constraint(values, pltpu.VMEM)


def split2(values):
    high = values.astype(BF16)
    return high, (values - high.astype(F32)).astype(BF16)


def split3(values):
    high = values.astype(BF16).astype(F32)
    rest = values - high
    middle = rest.astype(BF16).astype(F32)
    return high, middle, (rest - middle).astype(BF16).astype(F32)


def dot(left, right, dims):
    return lax.dot_general(left, right, dims, preferred_element_type=F32)


def stack2(values):
    high, low = split2(values)
    return jnp.concatenate([high, low], axis=0)


def dot3(left, right, dims):
    rows = left.shape[0] // 2
    wide = dot(left, right[0], dims)
    return wide[:rows] + wide[rows:] + dot(left[:rows], right[1], dims)


def by_kind(kind, table, empty=0.0):
    result = jnp.full(kind.shape, empty, F32)
    for kind_index in range(NSPEC):
        result = jnp.where(kind == float(kind_index), table[kind_index], result)
    return result


def real_basis(length):
    rows = np.arange(length)[:, None]
    points = np.arange(length)[None, :]
    half = length // 2
    waves = np.where(rows <= half, rows, length - rows)
    angle = 2.0 * np.pi * ((waves * points) % length) / length
    basis = np.where(rows <= half, np.cos(angle), np.sin(angle)) * math.sqrt(2.0 / length)
    basis[0] *= math.sqrt(0.5)
    basis[half] *= math.sqrt(0.5)
    return basis


def table_pair(values):
    values = values.astype(np.float32)
    high = values.astype(ml_dtypes.bfloat16)
    low = (values - high.astype(np.float32)).astype(ml_dtypes.bfloat16)
    return jnp.asarray(np.stack([high, low]))


def signed_modes(indices, total):
    return jnp.where(2 * indices >= total, indices - total, indices)


def chunk_transpose(tiles, chunk):
    tiles = list(tiles)
    count = len(tiles)
    width = tiles[0].shape[-1]
    lane_chunk = lax.broadcasted_iota(jnp.int32, tiles[0].shape, 1) // chunk
    bit = 1
    while bit < count:
        keep = (lane_chunk & bit) == 0
        for low in range(count):
            if low & bit:
                continue
            first, second = tiles[low], tiles[low | bit]
            tiles[low] = jnp.where(keep, first, pltpu.roll(second, bit * chunk, 1))
            tiles[low | bit] = jnp.where(keep, pltpu.roll(first, width - bit * chunk, 1), second)
        bit *= 2
    return tiles


def point_weights(offset_row, fraction_row):
    points = lax.broadcasted_iota(jnp.int32, (PPC, offset_row.shape[-1]), 0).astype(F32)
    lower = points == offset_row
    upper = points == offset_row + 1.0
    weights = jnp.where(lower, 1.0 - fraction_row, jnp.where(upper, fraction_row, 0.0))
    slopes = jnp.where(lower, -1.0, jnp.where(upper, 1.0, 0.0))
    return weights, slopes


def make_spread(parts, cells_y, cells_z, slots, lz, devices, relayout):
    columns = parts * cells_z
    modes = lz // devices
    yl = cells_y * PPC
    rows = PPC * PPC

    tiles = lz // 128
    reach = columns // tiles

    def kernel(atoms, table, basis_any, out_any, plane, line, basis_ref, out, sem, sends):
        fetch = pltpu.make_async_copy(basis_any, basis_ref, sem)
        fetch.start()
        line[...] = jnp.zeros(line.shape, BF16)
        pieces = []
        for cy in range(cells_y):
            brick = []
            for tile in range(tiles):
                for place in range(reach):
                    column = tile * reach + place
                    cell = atoms[column // cells_z, cy, :, column % cells_z, :]
                    weights = [
                        point_weights(cell[d : d + 1], cell[3 + d : 4 + d])[0] for d in range(3)
                    ]
                    along_x = weights[0] * by_kind(cell[6:7], table)
                    value = jnp.concatenate(
                        [weights[1][y : y + 1] * along_x for y in range(PPC)], axis=0
                    )
                    lanes = pl.ds(place * slots, slots)
                    high, low = split2(value)
                    plane[tile, pl.ds(0, rows), lanes] = high
                    plane[tile, pl.ds(rows, rows), lanes] = low
                    high, low = split2(weights[2])
                    line[tile, pl.ds(place * PPC, PPC), lanes] = high
                    line[tile, pl.ds(128 + place * PPC, PPC), lanes] = low
                wide = dot(plane[tile], line[tile], NT)
                wide = wide[:rows] + wide[rows:]
                brick.append(wide[:, :128] + wide[:, 128:])
            if cy == 0:
                fetch.wait()
            brick = jnp.concatenate(brick, axis=1)
            pieces.append(dot3(stack2(brick), (basis_ref[0], basis_ref[1]), NT))
        if not relayout:
            for cy in range(cells_y):
                out[pl.ds(cy * rows, rows), :] = pieces[cy]
            copy = pltpu.make_async_copy(out, out_any, sends.at[0])
            copy.start()
            copy.wait()
            return
        chunks = 128 // modes
        copies = []
        for tile in range(tiles):
            for group in range(yl // chunks):
                parts = []
                for y in range(group * chunks, (group + 1) * chunks):
                    start = (y % PPC) * PPC
                    parts.append(
                        pieces[y // PPC][start : start + PPC, tile * 128 : tile * 128 + 128]
                    )
                for chunk, value in enumerate(chunk_transpose(parts, modes)):
                    out[tile * chunks + chunk, :, pl.ds(group * 128, 128)] = value
            there = pl.ds(tile * chunks, chunks)
            copies.append(pltpu.make_async_copy(out.at[there], out_any.at[there], sends.at[tile]))
            copies[-1].start()
        for copy in copies:
            copy.wait()

    if relayout:
        shape = (devices, PPC, yl * modes)
    else:
        shape = (cells_y * rows, lz)
    return pl.pallas_call(
        kernel,
        out_shape=jax.ShapeDtypeStruct(shape, F32),
        in_specs=[VMEM, SMEM, ANY],
        out_specs=ANY,
        scratch_shapes=[
            pltpu.VMEM((tiles, 2 * rows, reach * slots), BF16),
            pltpu.VMEM((tiles, 256, reach * slots), BF16),
            pltpu.VMEM((2, lz, lz), BF16),
            pltpu.VMEM(shape, F32),
            pltpu.SemaphoreType.DMA(()),
            pltpu.SemaphoreType.DMA((tiles,)),
        ],
        compiler_params=PARAMS,
        name="spread",
    )


def make_planes(gx, gy, gz, lanes, lx, ly, lz):
    modes = lz // (gx * gy * gz)
    width = ly * modes
    sharp = -1.0 / (4.0 * EWALD_SPLIT * EWALD_SPLIT)

    def wave_square(indices, length):
        return jnp.square(signed_modes(indices, length).astype(F32) * (2.0 * math.pi / length))

    def kernel(
        rank, data, x_any, xt_any, y_any, out_any, grid, x_ref, xt_ref, y_ref, out, sems, sends
    ):
        fetches = [
            pltpu.make_async_copy(source, target, sems.at[index])
            for index, (source, target) in enumerate(
                ((x_any, x_ref), (y_any, y_ref), (xt_any, xt_ref))
            )
        ]
        for fetch in fetches:
            fetch.start()
        for a in range(gx):
            for b in range(gy):
                for c in range(gz):
                    grid[pl.ds((a * gz + c) * PPC, PPC), pl.ds(b * lanes, lanes)] = data[
                        (a * gy + b) * gz + c
                    ]
        lane = lax.broadcasted_iota(jnp.int32, (1, width), 1)
        across = wave_square(lane // modes, ly) + wave_square(rank[0] * modes + lane % modes, lz)
        along = wave_square(lax.broadcasted_iota(jnp.int32, (lx, 1), 0), lx)
        squared = along + across
        factor = (4.0 * math.pi * jnp.exp(along * sharp)) * jnp.exp(across * sharp)
        green = jnp.where(squared == 0.0, 0.0, factor / jnp.where(squared == 0.0, 1.0, squared))
        fetches[0].wait()
        value = dot3(x_ref[...], split2(grid[...]), NN)
        fetches[1].wait()
        value = dot3(stack2(value), (y_ref[0], y_ref[1]), NT) * green
        value = dot3(stack2(value), (y_ref[0], y_ref[1]), NN)
        fetches[2].wait()
        copies = []
        for b in range(gy):
            part = dot3(xt_ref[...], split2(value[:, b * lanes : (b + 1) * lanes]), NN)
            for a in range(gx):
                first = (a * gy + b) * gz
                for c in range(gz):
                    start = (a * gz + c) * PPC
                    out[first + c] = part[start : start + PPC]
                there = pl.ds(first, gz)
                copies.append(
                    pltpu.make_async_copy(out.at[there], out_any.at[there], sends.at[len(copies)])
                )
                copies[-1].start()
        for copy in copies:
            copy.wait()

    return pl.pallas_call(
        kernel,
        out_shape=jax.ShapeDtypeStruct((gx * gy * gz, PPC, lanes), F32),
        in_specs=[SMEM, VMEM, ANY, ANY, ANY],
        out_specs=ANY,
        scratch_shapes=[
            pltpu.VMEM((lx, width), F32),
            pltpu.VMEM((2 * lx, lx), BF16),
            pltpu.VMEM((2 * lx, lx), BF16),
            pltpu.VMEM((2, width, width), BF16),
            pltpu.VMEM((gx * gy * gz, PPC, lanes), F32),
            pltpu.SemaphoreType.DMA((3,)),
            pltpu.SemaphoreType.DMA((gx * gy,)),
        ],
        compiler_params=PARAMS,
        name="planes",
    )


def make_sample(parts, cells_y, cells_z, slots, lz, devices, relayout):
    columns = parts * cells_z
    modes = lz // devices
    yl = cells_y * PPC
    rows = PPC * PPC

    reach = columns * 128 // lz

    def kernel(
        data, atoms, short, dens, table, basis_any, out, lines, line, basis_ref, sem
    ):
        fetch = pltpu.make_async_copy(basis_any, basis_ref, sem)
        fetch.start()
        if relayout:
            chunks = 128 // modes
            for tile in range(lz // 128):
                for group in range(yl // chunks):
                    tiles = [
                        data[tile * chunks + chunk, :, pl.ds(group * 128, 128)]
                        for chunk in range(chunks)
                    ]
                    for index, value in enumerate(chunk_transpose(tiles, modes)):
                        lines[
                            pl.ds((group * chunks + index) * PPC, PPC), pl.ds(tile * 128, 128)
                        ] = value
        else:
            lines[...] = data[...]
        line[...] = jnp.zeros(line.shape, BF16)
        fetch.wait()
        for cy in range(cells_y):
            brick = dot3(
                stack2(lines[pl.ds(cy * rows, rows), :]), (basis_ref[0], basis_ref[1]), NN
            )
            for column in range(columns):
                if column % reach == 0:
                    start = column // reach * 128
                    value = brick[:, start : start + 128]
                    high = value.astype(BF16)
                    left_half = lax.broadcasted_iota(jnp.int32, value.shape, 1) < 64
                    top = high.astype(F32)
                    swapped = pltpu.roll(value - top, 64, 1)
                    wides = [
                        jnp.concatenate([half.astype(BF16), high], axis=1)
                        for half in (
                            jnp.where(left_half, top, swapped),
                            jnp.where(left_half, swapped, top),
                        )
                    ]
                wide = wides[column % reach * 2 // reach]
                cell = atoms[column // cells_z, cy, :, column % cells_z, :]
                pairs = [point_weights(cell[d : d + 1], cell[3 + d : 4 + d]) for d in range(3)]
                (wx, sx), (wy, sy), (wz, sz) = pairs
                first = column % reach * PPC
                high, low = split2(wz)
                both = jnp.concatenate([high, sz.astype(BF16)], axis=1)
                line[column, pl.ds(first, PPC), :] = both
                line[column, pl.ds((first + 64) % 128, PPC), :] = both
                line[column, pl.ds(128 + first, PPC), pl.ds(0, slots)] = low
                both = dot(wide, line[column], NN)
                plain, tilted = both[:, :slots], both[:, slots:]
                force_x = jnp.zeros((PPC, slots), F32)
                force_y = jnp.zeros((PPC, slots), F32)
                force_z = jnp.zeros((PPC, slots), F32)
                for y in range(PPC):
                    block = plain[y * PPC : (y + 1) * PPC]
                    force_x += wy[y : y + 1] * block
                    force_y += sy[y : y + 1] * block
                    force_z += wy[y : y + 1] * tilted[y * PPC : (y + 1) * PPC]
                charge = -COUPLING * by_kind(cell[6:7], table)
                here = pl.ds(column, 1)
                result = [
                    charge * jnp.sum(force * weight, axis=0, keepdims=True)
                    + short[d, cy, here, :]
                    for d, (force, weight) in enumerate(
                        ((force_x, sx), (force_y, wx), (force_z, wx))
                    )
                ]
                result = [jnp.where(cell[6:7] >= 0.0, value, 0.0) for value in result]
                result.append(dens[cy, here, :])
                out[column // cells_z, cy, :, column % cells_z, :] = jnp.concatenate(result, axis=0)

    return pl.pallas_call(
        kernel,
        out_shape=pltpu.VMEM((parts, cells_y, 4, cells_z, slots), F32),
        in_specs=[VMEM, VMEM, VMEM, VMEM, SMEM, ANY],
        out_specs=VMEM,
        scratch_shapes=[
            pltpu.VMEM((cells_y * rows, lz), F32),
            pltpu.VMEM((columns, 256, 2 * slots), BF16),
            pltpu.VMEM((2, lz, lz), BF16),
            pltpu.SemaphoreType.DMA(()),
        ],
        compiler_params=PARAMS,
        name="sample",
    )


def make_finish(shape):
    cells_x, cells_y, _, cells_z, slots = shape

    def kernel(result, forces, density, sems):
        copies = [
            pltpu.make_async_copy(result.at[:, :, pl.ds(0, 3)], forces, sems.at[0]),
            pltpu.make_async_copy(result.at[:, :, 3], density, sems.at[1]),
        ]
        for copy in copies:
            copy.start()
        for copy in copies:
            copy.wait()

    return pl.pallas_call(
        kernel,
        out_shape=(
            jax.ShapeDtypeStruct((cells_x, cells_y, 3, cells_z, slots), F32),
            jax.ShapeDtypeStruct((cells_x, cells_y, cells_z, slots), F32),
        ),
        in_specs=[VMEM],
        out_specs=(ANY, ANY),
        scratch_shapes=[pltpu.SemaphoreType.DMA((2,))],
        compiler_params=PARAMS,
        name="finish",
    )


RIGHT = ((0, 0), (1, 0), (1, 0), (2, 0))
LEFT = ((0, 1), (0, 1), (1, 2), (0, 2))


def clear_spare(ref):
    count = ref.shape[1] // 8
    for tile in (1, 3):
        ref[tile, pl.ds(7, count, stride=8), :] = jnp.zeros((count, ref.shape[2]), F32)


def store_five(ref, first, count, values, order):
    pieces = [split3(value) for value in values]
    for tile, (main, third) in enumerate(order):
        rows = [pieces[index][main] for index in range(5)]
        rows += [pieces[index][third] for index in ((3, 4) if tile % 2 else (0, 1, 2))]
        for row, value in enumerate(rows):
            ref[tile, pl.ds(first * 8 + row, count, stride=8), :] = value


def five_rows(ref, cell):
    tiles = [ref[tile, pl.ds(cell * 8, 8), :] for tile in range(4)]
    return jnp.concatenate(tiles, axis=0).astype(BF16)


def fill(feature, own_feature, right, left):
    def fill_right(n, carry):
        right[n] = five_rows(feature, n)
        return carry

    def fill_left(n, carry):
        left[n] = five_rows(own_feature, n).T
        return carry

    lax.fori_loop(0, right.shape[0], fill_right, 0, unroll=8)
    lax.fori_loop(0, left.shape[0], fill_left, 0, unroll=8)


def two_rows(values, side):
    high = values.astype(BF16).astype(F32)
    rest = values - high
    row = lax.broadcasted_iota(jnp.int32, values.shape, 0)
    pick = row < 4 if side else row % 4 < 2
    return jnp.concatenate([jnp.where(pick, high, rest), jnp.zeros_like(values)], axis=0)


def channel(block, y, nz, index):
    return block[pl.ds((y * 4 + index) * nz, nz), :]


def row_positions(block, x, y, sy, nz):
    pos_x = channel(block, y, nz, 0) + (x - 1.0)
    pos_y = channel(block, y, nz, 1) + (y - 0.5 * (sy - 1))
    return pos_x, pos_y, channel(block, y, nz, 2)


def same_slot(slots):
    return lax.broadcasted_iota(jnp.int32, (slots, slots), 0) == lax.broadcasted_iota(
        jnp.int32, (slots, slots), 1
    )


def make_density(cells_y, nz, slots):
    sy = cells_y + 2
    own = cells_y * nz
    total = 3 * sy * nz

    def kernel(
        low, mid, high, electrons, embed, density, slope, feature, own_feature, right, left, sums
    ):
        clear_spare(feature)
        clear_spare(own_feature)
        for x, block in enumerate((low, mid, high)):
            for y in range(sy):
                pos = row_positions(block, x, y, sy, nz)
                square = pos[0] * pos[0] + pos[1] * pos[1] + pos[2] * pos[2]
                kind = channel(block, y, nz, 3)
                scale = jnp.exp(jnp.log(by_kind(kind, electrons, 1.0)) * (1.0 / 3.0))
                scale = jnp.where(kind >= 0.0, scale, 0.0)
                double = 2.0 * scale
                values = [scale * (1.0 - square)] + [double * pos[d] for d in range(3)] + [-scale]
                store_five(feature, (x * sy + y) * nz, nz, values, RIGHT)
                if x == 1 and 1 <= y <= cells_y:
                    for dz in range(3):
                        across = pos[2] - (dz - 1.0)
                        square = pos[0] * pos[0] + pos[1] * pos[1] + across * across
                        values = [jnp.ones_like(square), pos[0], pos[1], across, square]
                        store_five(own_feature, dz * own + (y - 1) * nz, nz, values, LEFT)

        fill(feature, own_feature, right, left)
        same = same_slot(slots)
        lane = lax.broadcasted_iota(jnp.int32, (slots, 128), 1)
        sums[...] = jnp.zeros(sums.shape, F32)

        def one_cell(n, carry):
            y, z = n // nz, n % nz
            weight = jnp.maximum(dot(left[own + n], right[(sy + y + 1) * nz + z], NN), 0.0)
            weight = jnp.where(same, 0.0, weight)
            total_sum = weight * weight * weight
            for dz in range(3):
                zz = (z + (dz - 1 + nz)) % nz
                lhs = left[dz * own + n]
                near = [(dx * sy + y + dy) * nz + zz for dx in range(3) for dy in range(3)]
                if dz == 1:
                    near.pop(4)
                while near:
                    pair, near = near[:2], near[2:]
                    rhs = [right[index] for index in pair]
                    rhs = jnp.concatenate(rhs, axis=1) if len(rhs) > 1 else rhs[0]
                    weight = jnp.maximum(dot(lhs, rhs, NN), 0.0)
                    cube = weight * weight * weight
                    for part in range(len(pair)):
                        total_sum = total_sum + cube[:, part * slots : (part + 1) * slots]
            column = jnp.sum(total_sum, axis=1, keepdims=True)
            sums[...] = jnp.where(lane == n, column, sums[...])
            return carry

        lax.fori_loop(0, own, one_cell, 0, unroll=4)
        rows = sums[...].T
        for y in range(cells_y):
            kind = channel(mid, y + 1, nz, 3)
            value = jnp.where(kind >= 0.0, rows[y * nz : (y + 1) * nz], 0.0)
            density[y] = value
            slope[pl.ds(y * nz, nz), :] = -by_kind(kind, embed) / (2.0 * jnp.sqrt(1.0 + value))

    return pl.pallas_call(
        kernel,
        out_shape=(
            pltpu.VMEM((cells_y, nz, slots), F32),
            pltpu.VMEM((own, slots), F32),
        ),
        in_specs=[VMEM, VMEM, VMEM, SMEM, SMEM],
        out_specs=(VMEM, VMEM),
        scratch_shapes=[
            pltpu.VMEM((4, total * 8, slots), F32),
            pltpu.VMEM((4, 3 * own * 8, slots), F32),
            pltpu.VMEM((total, 32, slots), BF16),
            pltpu.VMEM((3 * own, slots, 32), BF16),
            pltpu.VMEM((slots, 128), F32),
        ],
        compiler_params=PARAMS,
        cost_estimate=pl.CostEstimate(
            flops=own * 27 * slots * slots * 40, bytes_accessed=total * slots * 16, transcendentals=0
        ),
        name="density",
    )


def make_force(cells_y, nz, slots):
    sy = cells_y + 2
    own = cells_y * nz
    total = 3 * sy * nz
    chunk = 8

    def kernel(
        low, mid, high, slope_low, slope_mid, slope_high, electrons, repel, out,
        feature, extra, own_feature, own_extra, place, right, right_extra, left, left_extra, acc, sums,
    ):
        clear_spare(feature)
        clear_spare(own_feature)
        blocks = zip((low, mid, high), (slope_low, slope_mid, slope_high))
        for x, (block, slopes) in enumerate(blocks):
            for y in range(sy):
                pos = row_positions(block, x, y, sy, nz)
                square = pos[0] * pos[0] + pos[1] * pos[1] + pos[2] * pos[2]
                kind = channel(block, y, nz, 3)
                scale = by_kind(kind, repel)
                inverse = 1.0 / by_kind(kind, repel, 1.0)
                inverse = inverse * inverse
                steep = slopes[pl.ds(y * nz, nz), :] * inverse
                mild = -3.0 * by_kind(kind, electrons) * inverse
                double = 2.0 * scale
                values = [scale * (1.0 - square)] + [double * pos[d] for d in range(3)] + [-scale]
                cell = (x * sy + y) * nz
                store_five(feature, cell, nz, values, RIGHT)
                for d in range(3):
                    place[pl.ds(cell * 8 + d, nz, stride=8), :] = pos[d]
                for k in range(8):
                    extra[pl.ds(cell * 8 + k, nz, stride=8), :] = mild if k % 2 else steep
                if x == 1 and 1 <= y <= cells_y:
                    cell = (y - 1) * nz
                    for k in range(8):
                        own_extra[pl.ds(cell * 8 + k, nz, stride=8), :] = steep if k % 2 else mild
                    for dz in range(3):
                        across = pos[2] - (dz - 1.0)
                        square = pos[0] * pos[0] + pos[1] * pos[1] + across * across
                        values = [scale] + [
                            scale * value for value in (pos[0], pos[1], across, square)
                        ]
                        store_five(own_feature, dz * own + cell, nz, values, LEFT)

        fill(feature, own_feature, right, left)

        def fill_right_extra(n, carry):
            right_extra[n] = two_rows(extra[pl.ds(n * 8, 8), :], 0).astype(BF16)
            return carry

        def fill_left_extra(n, carry):
            left_extra[n] = two_rows(own_extra[pl.ds(n * 8, 8), :], 1).astype(BF16).T
            return carry

        lax.fori_loop(0, total, fill_right_extra, 0, unroll=8)
        lax.fori_loop(0, own, fill_left_extra, 0, unroll=8)
        same = same_slot(slots)
        lane = lax.broadcasted_iota(jnp.int32, (slots, 128), 1)
        sums[...] = jnp.zeros(sums.shape, F32)

        def one_cell(n, carry):
            y, z = n // nz, n % nz
            lhs_extra = left_extra[n]
            first = True
            for dz in range(3):
                zz = (z + (dz - 1 + nz)) % nz
                lhs = left[dz * own + n]
                near = [(dx * sy + y + dy) * nz + zz for dx in range(3) for dy in range(3)]
                if dz == 1:
                    near.append(near.pop(4))
                for index in range(0, 9, 2):
                    pair = near[index : index + 2]
                    rhs = [right[cell] for cell in pair]
                    rhs_extra = [right_extra[cell] for cell in pair]
                    if len(pair) > 1:
                        rhs = [jnp.concatenate(rhs, axis=1)]
                        rhs_extra = [jnp.concatenate(rhs_extra, axis=1)]
                    bare = dot(lhs, rhs[0], NN)
                    value = bare * dot(lhs_extra, rhs_extra[0], NN) - 2.0
                    weight = jnp.maximum(bare, 0.0)
                    if dz == 1 and index == 8:
                        weight = jnp.where(same, 0.0, weight)
                    value = value * weight
                    there = [
                        [place[pl.ds(cell * 8 + d, 1), :] for d in range(3)] for cell in pair
                    ]
                    if dz != 1:
                        there = [[x, y_, z_ + (dz - 1.0)] for x, y_, z_ in there]
                    for start in range(0, slots, chunk):
                        rows = pl.ds(start, chunk)
                        tiles = [
                            value[start : start + chunk, k * slots : (k + 1) * slots]
                            for k in range(len(pair))
                        ]
                        sums_of = [
                            [tile * there[k][d] for k, tile in enumerate(tiles)] for d in range(3)
                        ] + [tiles]
                        for d in range(4):
                            part = sums_of[d][0]
                            for more in sums_of[d][1:]:
                                part = part + more
                            acc[d, rows, :] = part if first else acc[d, rows, :] + part
                    first = False
            for d in range(4):
                column = jnp.sum(acc[d], axis=1, keepdims=True)
                sums[d] = jnp.where(lane == n, column, sums[d])
            return carry

        lax.fori_loop(0, own, one_cell, 0, unroll=8)
        rows = [sums[d].T for d in range(4)]
        for y in range(cells_y):
            pos = row_positions(mid, 1, y + 1, sy, nz)
            part = slice(y * nz, (y + 1) * nz)
            for d in range(3):
                out[d, y] = 2.0 * (rows[d][part] - pos[d] * rows[3][part])

    return pl.pallas_call(
        kernel,
        out_shape=pltpu.VMEM((3, cells_y, nz, slots), F32),
        in_specs=[VMEM] * 6 + [SMEM, SMEM],
        out_specs=VMEM,
        scratch_shapes=[
            pltpu.VMEM((4, total * 8, slots), F32),
            pltpu.VMEM((total * 8, slots), F32),
            pltpu.VMEM((4, 3 * own * 8, slots), F32),
            pltpu.VMEM((own * 8, slots), F32),
            pltpu.VMEM((total * 8, slots), F32),
            pltpu.VMEM((total, 32, slots), BF16),
            pltpu.VMEM((total, 16, slots), BF16),
            pltpu.VMEM((3 * own, slots, 32), BF16),
            pltpu.VMEM((own, slots, 16), BF16),
            pltpu.VMEM((4, slots, slots), F32),
            pltpu.VMEM((4, slots, 128), F32),
        ],
        compiler_params=PARAMS,
        cost_estimate=pl.CostEstimate(
            flops=own * 27 * slots * slots * 100,
            bytes_accessed=total * slots * 16,
            transcendentals=0,
        ),
        name="force",
    )


def shifted(axis, count):
    up = [(i, (i + 1) % count) for i in range(count)]
    down = [(target, source) for source, target in up]
    return lambda part: lax.ppermute(part, axis, up), lambda part: lax.ppermute(part, axis, down)


def halo(block, rows, gx, gy, gz):
    up, down = shifted("gy", gy)
    if gy == 2 and block.shape[0] == 2 * rows:
        other = up(block)
        low, high = other[-rows:], other[:rows]
    else:
        low, high = up(block[-rows:]), down(block[:rows])
    middle = jnp.concatenate([low, block, high], axis=0)
    up, down = shifted(("gx", "gz"), gx * gz)
    low = up(middle)
    high = down(middle)
    return low, middle, high


def on_device(
    cell_counts,
    grid_offset,
    fraction,
    species,
    species_density,
    species_pair,
    species_embed,
    species_charge,
):
    cells_x, cells_y, cells_z, _, slots = fraction.shape
    gx, gy, gz = (lax.axis_size(name) for name in ("gx", "gy", "gz"))
    devices = gx * gy * gz
    assert cells_x == gz and slots == 128
    lx, ly, lz = cells_x * gx * PPC, cells_y * gy * PPC, cells_z * gz * PPC
    assert lz % devices == 0
    modes = lz // devices
    yl = cells_y * PPC
    relayout = modes <= 128 and yl % max(1, 128 // modes) == 0

    slot_index = lax.broadcasted_iota(jnp.int32, species.shape, 3)
    alive = slot_index < cell_counts[..., None]
    kind = jnp.where(alive, species.astype(F32), -1.0)[:, :, None]

    atoms = jnp.concatenate(
        [
            grid_offset.astype(F32).transpose(0, 1, 3, 2, 4),
            fraction.transpose(0, 1, 3, 2, 4),
            kind,
        ],
        axis=2,
    )
    atoms = lax.all_to_all(atoms, "gz", split_axis=0, concat_axis=0, tiled=True)
    basis_x, basis_z = real_basis(lx), real_basis(lz)
    x_pair, xt_pair, z_pair = table_pair(basis_x), table_pair(basis_x.T), table_pair(basis_z)
    y_pair = table_pair(np.kron(real_basis(ly), np.eye(modes)))
    spread = make_spread(gz, cells_y, cells_z, slots, lz, devices, relayout)
    lines = spread(near_core(atoms), species_charge, z_pair)
    if not relayout:
        lines = lines.reshape(yl, PPC, devices, modes).transpose(2, 1, 0, 3)
        lines = lines.reshape(devices, PPC, yl * modes)
    planes = lax.all_to_all(lines, ("gx", "gy", "gz"), split_axis=0, concat_axis=0, tiled=True)

    nz = gz * cells_z
    place = (atoms[:, :, 0:3] + 0.5 + atoms[:, :, 3:6]) / PPC - 0.5
    place = jnp.concatenate([place, atoms[:, :, 6:7]], axis=2)
    place = place.transpose(1, 2, 0, 3, 4).reshape(cells_y * 4 * nz, slots)
    near = halo(place, nz * 4, gx, gy, gz)
    density, slope = make_density(cells_y, nz, slots)(
        *map(near_core, near), species_density, species_embed
    )
    near_slopes = halo(slope, nz, gx, gy, gz)

    rank = lax.axis_index(("gx", "gy", "gz")).astype(jnp.int32).reshape(1)
    planes = make_planes(gx, gy, gz, yl * modes, lx, ly, lz)(
        rank, near_core(planes), x_pair.reshape(2 * lx, lx), xt_pair.reshape(2 * lx, lx), y_pair
    )
    lines = lax.all_to_all(planes, ("gx", "gy", "gz"), split_axis=0, concat_axis=0, tiled=True)
    if not relayout:
        lines = lines.reshape(devices, PPC, yl, modes).transpose(2, 1, 0, 3)
        lines = lines.reshape(yl * PPC, lz)

    operands = (*near, *near_slopes)
    short = make_force(cells_y, nz, slots)(*map(near_core, operands), species_density, species_pair)
    result = make_sample(gz, cells_y, cells_z, slots, lz, devices, relayout)(
        near_core(lines), near_core(atoms), near_core(short), near_core(density), species_charge, z_pair
    )
    result = lax.all_to_all(result, "gz", split_axis=0, concat_axis=0, tiled=True)
    forces, density = make_finish(result.shape)(near_core(result))
    return (forces.transpose(0, 1, 3, 2, 4), density)


def solution(mesh):
    return jax.shard_map(
        on_device,
        mesh=mesh,
        in_specs=(
            P("gx", "gy", "gz"),
            P("gx", "gy", "gz", None, None),
            P("gx", "gy", "gz", None, None),
            P("gx", "gy", "gz", None),
            P(),
            P(),
            P(),
            P(),
        ),
        out_specs=(P("gx", "gy", "gz", None, None), P("gx", "gy", "gz", None)),
        check_vma=False,
    )
```

```python
import math

import ml_dtypes
import numpy as np

import jax
import jax.numpy as jnp
from jax import lax
from jax.experimental import pallas as pl
from jax.experimental.pallas import tpu as pltpu
from jax.sharding import PartitionSpec as P


NSPEC = 2
PPC = 16
EWALD_SPLIT = 0.7
COUPLING = 8.0
F32 = jnp.float32
BF16 = jnp.bfloat16
VMEM = pl.BlockSpec(memory_space=pltpu.VMEM)
SMEM = pl.BlockSpec(memory_space=pltpu.SMEM)
ANY = pl.BlockSpec(memory_space=pl.ANY)
NN = (((1,), (0,)), ((), ()))
NT = (((1,), (1,)), ((), ()))
PARAMS = pltpu.CompilerParams(vmem_limit_bytes=56 * 1024 * 1024)


def near_core(values):
    return pltpu.with_memory_space_constraint(values, pltpu.VMEM)


def split2(values):
    high = values.astype(BF16)
    return high, (values - high.astype(F32)).astype(BF16)


def split3(values):
    high = values.astype(BF16).astype(F32)
    rest = values - high
    middle = rest.astype(BF16).astype(F32)
    return high, middle, (rest - middle).astype(BF16).astype(F32)


def dot(left, right, dims):
    return lax.dot_general(left, right, dims, preferred_element_type=F32)


def stack2(values):
    high, low = split2(values)
    return jnp.concatenate([high, low], axis=0)


def dot3(left, right, dims):
    rows = left.shape[0] // 2
    wide = dot(left, right[0], dims)
    return wide[:rows] + wide[rows:] + dot(left[:rows], right[1], dims)


def by_kind(kind, table, empty=0.0):
    result = jnp.full(kind.shape, empty, F32)
    for kind_index in range(NSPEC):
        result = jnp.where(kind == float(kind_index), table[kind_index], result)
    return result


def real_basis(length):
    rows = np.arange(length)[:, None]
    points = np.arange(length)[None, :]
    half = length // 2
    waves = np.where(rows <= half, rows, length - rows)
    angle = 2.0 * np.pi * ((waves * points) % length) / length
    basis = np.where(rows <= half, np.cos(angle), np.sin(angle)) * math.sqrt(2.0 / length)
    basis[0] *= math.sqrt(0.5)
    basis[half] *= math.sqrt(0.5)
    return basis


def table_pair(values):
    values = values.astype(np.float32)
    high = values.astype(ml_dtypes.bfloat16)
    low = (values - high.astype(np.float32)).astype(ml_dtypes.bfloat16)
    return jnp.asarray(np.stack([high, low]))


def signed_modes(indices, total):
    return jnp.where(2 * indices >= total, indices - total, indices)


def chunk_transpose(tiles, chunk):
    tiles = list(tiles)
    count = len(tiles)
    width = tiles[0].shape[-1]
    lane_chunk = lax.broadcasted_iota(jnp.int32, tiles[0].shape, 1) // chunk
    bit = 1
    while bit < count:
        keep = (lane_chunk & bit) == 0
        for low in range(count):
            if low & bit:
                continue
            first, second = tiles[low], tiles[low | bit]
            tiles[low] = jnp.where(keep, first, pltpu.roll(second, bit * chunk, 1))
            tiles[low | bit] = jnp.where(keep, pltpu.roll(first, width - bit * chunk, 1), second)
        bit *= 2
    return tiles


def point_weights(offset_row, fraction_row):
    points = lax.broadcasted_iota(jnp.int32, (PPC, offset_row.shape[-1]), 0).astype(F32)
    lower = points == offset_row
    upper = points == offset_row + 1.0
    weights = jnp.where(lower, 1.0 - fraction_row, jnp.where(upper, fraction_row, 0.0))
    slopes = jnp.where(lower, -1.0, jnp.where(upper, 1.0, 0.0))
    return weights, slopes


def make_spread(parts, cells_y, cells_z, slots, lz, devices, relayout):
    columns = parts * cells_z
    modes = lz // devices
    yl = cells_y * PPC
    rows = PPC * PPC

    tiles = lz // 128
    reach = columns // tiles

    def kernel(atoms, table, basis_any, out_any, plane, line, basis_ref, out, sem, sends):
        fetch = pltpu.make_async_copy(basis_any, basis_ref, sem)
        fetch.start()
        line[...] = jnp.zeros(line.shape, BF16)
        pieces = []
        for cy in range(cells_y):
            brick = []
            for tile in range(tiles):
                for place in range(reach):
                    column = tile * reach + place
                    cell = atoms[column // cells_z, cy, :, column % cells_z, :]
                    weights = [
                        point_weights(cell[d : d + 1], cell[3 + d : 4 + d])[0] for d in range(3)
                    ]
                    along_x = weights[0] * by_kind(cell[6:7], table)
                    value = jnp.concatenate(
                        [weights[1][y : y + 1] * along_x for y in range(PPC)], axis=0
                    )
                    lanes = pl.ds(place * slots, slots)
                    high, low = split2(value)
                    plane[tile, pl.ds(0, rows), lanes] = high
                    plane[tile, pl.ds(rows, rows), lanes] = low
                    high, low = split2(weights[2])
                    line[tile, pl.ds(place * PPC, PPC), lanes] = high
                    line[tile, pl.ds(128 + place * PPC, PPC), lanes] = low
                wide = dot(plane[tile], line[tile], NT)
                wide = wide[:rows] + wide[rows:]
                brick.append(wide[:, :128] + wide[:, 128:])
            if cy == 0:
                fetch.wait()
            brick = jnp.concatenate(brick, axis=1)
            pieces.append(dot3(stack2(brick), (basis_ref[0], basis_ref[1]), NT))
        if not relayout:
            for cy in range(cells_y):
                out[pl.ds(cy * rows, rows), :] = pieces[cy]
            copy = pltpu.make_async_copy(out, out_any, sends.at[0])
            copy.start()
            copy.wait()
            return
        chunks = 128 // modes
        copies = []
        for tile in range(tiles):
            for group in range(yl // chunks):
                parts = []
                for y in range(group * chunks, (group + 1) * chunks):
                    start = (y % PPC) * PPC
                    parts.append(
                        pieces[y // PPC][start : start + PPC, tile * 128 : tile * 128 + 128]
                    )
                for chunk, value in enumerate(chunk_transpose(parts, modes)):
                    out[tile * chunks + chunk, :, pl.ds(group * 128, 128)] = value
            there = pl.ds(tile * chunks, chunks)
            copies.append(pltpu.make_async_copy(out.at[there], out_any.at[there], sends.at[tile]))
            copies[-1].start()
        for copy in copies:
            copy.wait()

    if relayout:
        shape = (devices, PPC, yl * modes)
    else:
        shape = (cells_y * rows, lz)
    return pl.pallas_call(
        kernel,
        out_shape=jax.ShapeDtypeStruct(shape, F32),
        in_specs=[VMEM, SMEM, ANY],
        out_specs=ANY,
        scratch_shapes=[
            pltpu.VMEM((tiles, 2 * rows, reach * slots), BF16),
            pltpu.VMEM((tiles, 256, reach * slots), BF16),
            pltpu.VMEM((2, lz, lz), BF16),
            pltpu.VMEM(shape, F32),
            pltpu.SemaphoreType.DMA(()),
            pltpu.SemaphoreType.DMA((tiles,)),
        ],
        compiler_params=PARAMS,
        name="spread",
    )


def make_planes(gx, gy, gz, lanes, lx, ly, lz):
    modes = lz // (gx * gy * gz)
    width = ly * modes
    sharp = -1.0 / (4.0 * EWALD_SPLIT * EWALD_SPLIT)

    def wave_square(indices, length):
        return jnp.square(signed_modes(indices, length).astype(F32) * (2.0 * math.pi / length))

    def kernel(
        rank, data, x_any, xt_any, y_ref, out_any, grid, x_ref, xt_ref, out, sems, sends
    ):
        fetches = [
            pltpu.make_async_copy(source, target, sems.at[index])
            for index, (source, target) in enumerate(
                ((x_any, x_ref), (xt_any, xt_ref))
            )
        ]
        for fetch in fetches:
            fetch.start()
        for a in range(gx):
            for b in range(gy):
                for c in range(gz):
                    grid[pl.ds((a * gz + c) * PPC, PPC), pl.ds(b * lanes, lanes)] = data[
                        (a * gy + b) * gz + c
                    ]
        lane = lax.broadcasted_iota(jnp.int32, (1, width), 1)
        across = wave_square(lane // modes, ly) + wave_square(rank[0] * modes + lane % modes, lz)
        along = wave_square(lax.broadcasted_iota(jnp.int32, (lx, 1), 0), lx)
        squared = along + across
        factor = (4.0 * math.pi * jnp.exp(along * sharp)) * jnp.exp(across * sharp)
        green = jnp.where(squared == 0.0, 0.0, factor / jnp.where(squared == 0.0, 1.0, squared))
        fetches[0].wait()
        value = dot3(x_ref[...], split2(grid[...]), NN)
        value = dot3(stack2(value), (y_ref[0], y_ref[1]), NT) * green
        value = dot3(stack2(value), (y_ref[0], y_ref[1]), NN)
        fetches[1].wait()
        copies = []
        for b in range(gy):
            part = dot3(xt_ref[...], split2(value[:, b * lanes : (b + 1) * lanes]), NN)
            for a in range(gx):
                first = (a * gy + b) * gz
                for c in range(gz):
                    start = (a * gz + c) * PPC
                    out[first + c] = part[start : start + PPC]
                there = pl.ds(first, gz)
                copies.append(
                    pltpu.make_async_copy(out.at[there], out_any.at[there], sends.at[len(copies)])
                )
                copies[-1].start()
        for copy in copies:
            copy.wait()

    return pl.pallas_call(
        kernel,
        out_shape=jax.ShapeDtypeStruct((gx * gy * gz, PPC, lanes), F32),
        in_specs=[SMEM, VMEM, ANY, ANY, VMEM],
        out_specs=ANY,
        scratch_shapes=[
            pltpu.VMEM((lx, width), F32),
            pltpu.VMEM((2 * lx, lx), BF16),
            pltpu.VMEM((2 * lx, lx), BF16),
            pltpu.VMEM((gx * gy * gz, PPC, lanes), F32),
            pltpu.SemaphoreType.DMA((2,)),
            pltpu.SemaphoreType.DMA((gx * gy,)),
        ],
        compiler_params=PARAMS,
        name="planes",
    )


def make_sample(parts, cells_y, cells_z, slots, lz, devices, relayout):
    columns = parts * cells_z
    modes = lz // devices
    yl = cells_y * PPC
    rows = PPC * PPC

    reach = columns * 128 // lz

    def kernel(
        data, atoms, short, dens, table, basis_any, out, lines, line, basis_ref, sem
    ):
        fetch = pltpu.make_async_copy(basis_any, basis_ref, sem)
        fetch.start()
        if relayout:
            chunks = 128 // modes
            for tile in range(lz // 128):
                for group in range(yl // chunks):
                    tiles = [
                        data[tile * chunks + chunk, :, pl.ds(group * 128, 128)]
                        for chunk in range(chunks)
                    ]
                    for index, value in enumerate(chunk_transpose(tiles, modes)):
                        lines[
                            pl.ds((group * chunks + index) * PPC, PPC), pl.ds(tile * 128, 128)
                        ] = value
        else:
            lines[...] = data[...]
        line[...] = jnp.zeros(line.shape, BF16)
        fetch.wait()
        for cy in range(cells_y):
            brick = dot3(
                stack2(lines[pl.ds(cy * rows, rows), :]), (basis_ref[0], basis_ref[1]), NN
            )
            for column in range(columns):
                if column % reach == 0:
                    start = column // reach * 128
                    value = brick[:, start : start + 128]
                    high = value.astype(BF16)
                    left_half = lax.broadcasted_iota(jnp.int32, value.shape, 1) < 64
                    top = high.astype(F32)
                    swapped = pltpu.roll(value - top, 64, 1)
                    wides = [
                        jnp.concatenate([half.astype(BF16), high], axis=1)
                        for half in (
                            jnp.where(left_half, top, swapped),
                            jnp.where(left_half, swapped, top),
                        )
                    ]
                wide = wides[column % reach * 2 // reach]
                cell = atoms[column // cells_z, cy, :, column % cells_z, :]
                pairs = [point_weights(cell[d : d + 1], cell[3 + d : 4 + d]) for d in range(3)]
                (wx, sx), (wy, sy), (wz, sz) = pairs
                first = column % reach * PPC
                high, low = split2(wz)
                both = jnp.concatenate([high, sz.astype(BF16)], axis=1)
                line[column, pl.ds(first, PPC), :] = both
                line[column, pl.ds((first + 64) % 128, PPC), :] = both
                line[column, pl.ds(128 + first, PPC), pl.ds(0, slots)] = low
                both = dot(wide, line[column], NN)
                plain, tilted = both[:, :slots], both[:, slots:]
                force_x = jnp.zeros((PPC, slots), F32)
                force_y = jnp.zeros((PPC, slots), F32)
                force_z = jnp.zeros((PPC, slots), F32)
                for y in range(PPC):
                    block = plain[y * PPC : (y + 1) * PPC]
                    force_x += wy[y : y + 1] * block
                    force_y += sy[y : y + 1] * block
                    force_z += wy[y : y + 1] * tilted[y * PPC : (y + 1) * PPC]
                charge = -COUPLING * by_kind(cell[6:7], table)
                here = pl.ds(column, 1)
                result = [
                    charge * jnp.sum(force * weight, axis=0, keepdims=True)
                    + short[d, cy, here, :]
                    for d, (force, weight) in enumerate(
                        ((force_x, sx), (force_y, wx), (force_z, wx))
                    )
                ]
                result = [jnp.where(cell[6:7] >= 0.0, value, 0.0) for value in result]
                result.append(dens[cy, here, :])
                out[column // cells_z, cy, :, column % cells_z, :] = jnp.concatenate(result, axis=0)

    return pl.pallas_call(
        kernel,
        out_shape=pltpu.VMEM((parts, cells_y, 4, cells_z, slots), F32),
        in_specs=[VMEM, VMEM, VMEM, VMEM, SMEM, ANY],
        out_specs=VMEM,
        scratch_shapes=[
            pltpu.VMEM((cells_y * rows, lz), F32),
            pltpu.VMEM((columns, 256, 2 * slots), BF16),
            pltpu.VMEM((2, lz, lz), BF16),
            pltpu.SemaphoreType.DMA(()),
        ],
        compiler_params=PARAMS,
        name="sample",
    )


def make_finish(shape):
    cells_x, cells_y, _, cells_z, slots = shape

    def kernel(result, forces, density, sems):
        copies = [
            pltpu.make_async_copy(result.at[:, :, pl.ds(0, 3)], forces, sems.at[0]),
            pltpu.make_async_copy(result.at[:, :, 3], density, sems.at[1]),
        ]
        for copy in copies:
            copy.start()
        for copy in copies:
            copy.wait()

    return pl.pallas_call(
        kernel,
        out_shape=(
            jax.ShapeDtypeStruct((cells_x, cells_y, 3, cells_z, slots), F32),
            jax.ShapeDtypeStruct((cells_x, cells_y, cells_z, slots), F32),
        ),
        in_specs=[VMEM],
        out_specs=(ANY, ANY),
        scratch_shapes=[pltpu.SemaphoreType.DMA((2,))],
        compiler_params=PARAMS,
        name="finish",
    )


RIGHT = ((0, 0), (1, 0), (1, 0), (2, 0))
LEFT = ((0, 1), (0, 1), (1, 2), (0, 2))


def clear_spare(ref):
    count = ref.shape[1] // 8
    for tile in (1, 3):
        ref[tile, pl.ds(7, count, stride=8), :] = jnp.zeros((count, ref.shape[2]), F32)


def store_five(ref, first, count, values, order):
    pieces = [split3(value) for value in values]
    for tile, (main, third) in enumerate(order):
        rows = [pieces[index][main] for index in range(5)]
        rows += [pieces[index][third] for index in ((3, 4) if tile % 2 else (0, 1, 2))]
        for row, value in enumerate(rows):
            ref[tile, pl.ds(first * 8 + row, count, stride=8), :] = value


def five_rows(ref, cell):
    tiles = [ref[tile, pl.ds(cell * 8, 8), :] for tile in range(4)]
    return jnp.concatenate(tiles, axis=0).astype(BF16)


def fill(feature, own_feature, right, left):
    def fill_right(n, carry):
        right[n] = five_rows(feature, n)
        return carry

    def fill_left(n, carry):
        left[n] = five_rows(own_feature, n).T
        return carry

    lax.fori_loop(0, right.shape[0], fill_right, 0, unroll=8)
    lax.fori_loop(0, left.shape[0], fill_left, 0, unroll=8)


def two_rows(values, side):
    high = values.astype(BF16).astype(F32)
    rest = values - high
    row = lax.broadcasted_iota(jnp.int32, values.shape, 0)
    pick = row < 4 if side else row % 4 < 2
    return jnp.concatenate([jnp.where(pick, high, rest), jnp.zeros_like(values)], axis=0)


def channel(block, y, nz, index):
    return block[pl.ds((y * 4 + index) * nz, nz), :]


def row_positions(block, x, y, sy, nz):
    pos_x = channel(block, y, nz, 0) + (x - 1.0)
    pos_y = channel(block, y, nz, 1) + (y - 0.5 * (sy - 1))
    return pos_x, pos_y, channel(block, y, nz, 2)


def same_slot(slots):
    return lax.broadcasted_iota(jnp.int32, (slots, slots), 0) == lax.broadcasted_iota(
        jnp.int32, (slots, slots), 1
    )


def make_density(cells_y, nz, slots):
    sy = cells_y + 2
    own = cells_y * nz
    total = 3 * sy * nz

    def kernel(
        low, mid, high, electrons, embed, density, slope, feature, own_feature, right, left, sums
    ):
        clear_spare(feature)
        clear_spare(own_feature)
        for x, block in enumerate((low, mid, high)):
            for y in range(sy):
                pos = row_positions(block, x, y, sy, nz)
                square = pos[0] * pos[0] + pos[1] * pos[1] + pos[2] * pos[2]
                kind = channel(block, y, nz, 3)
                scale = jnp.exp(jnp.log(by_kind(kind, electrons, 1.0)) * (1.0 / 3.0))
                scale = jnp.where(kind >= 0.0, scale, 0.0)
                double = 2.0 * scale
                values = [scale * (1.0 - square)] + [double * pos[d] for d in range(3)] + [-scale]
                store_five(feature, (x * sy + y) * nz, nz, values, RIGHT)
                if x == 1 and 1 <= y <= cells_y:
                    for dz in range(3):
                        across = pos[2] - (dz - 1.0)
                        square = pos[0] * pos[0] + pos[1] * pos[1] + across * across
                        values = [jnp.ones_like(square), pos[0], pos[1], across, square]
                        store_five(own_feature, dz * own + (y - 1) * nz, nz, values, LEFT)

        fill(feature, own_feature, right, left)
        same = same_slot(slots)
        lane = lax.broadcasted_iota(jnp.int32, (slots, 128), 1)
        sums[...] = jnp.zeros(sums.shape, F32)

        def one_cell(n, carry):
            y, z = n // nz, n % nz
            weight = jnp.maximum(dot(left[own + n], right[(sy + y + 1) * nz + z], NN), 0.0)
            weight = jnp.where(same, 0.0, weight)
            total_sum = weight * weight * weight
            for dz in range(3):
                zz = (z + (dz - 1 + nz)) % nz
                lhs = left[dz * own + n]
                near = [(dx * sy + y + dy) * nz + zz for dx in range(3) for dy in range(3)]
                if dz == 1:
                    near.pop(4)
                while near:
                    pair, near = near[:2], near[2:]
                    rhs = [right[index] for index in pair]
                    rhs = jnp.concatenate(rhs, axis=1) if len(rhs) > 1 else rhs[0]
                    weight = jnp.maximum(dot(lhs, rhs, NN), 0.0)
                    cube = weight * weight * weight
                    for part in range(len(pair)):
                        total_sum = total_sum + cube[:, part * slots : (part + 1) * slots]
            column = jnp.sum(total_sum, axis=1, keepdims=True)
            sums[...] = jnp.where(lane == n, column, sums[...])
            return carry

        lax.fori_loop(0, own, one_cell, 0, unroll=4)
        rows = sums[...].T
        for y in range(cells_y):
            kind = channel(mid, y + 1, nz, 3)
            value = jnp.where(kind >= 0.0, rows[y * nz : (y + 1) * nz], 0.0)
            density[y] = value
            slope[pl.ds(y * nz, nz), :] = -by_kind(kind, embed) / (2.0 * jnp.sqrt(1.0 + value))

    return pl.pallas_call(
        kernel,
        out_shape=(
            pltpu.VMEM((cells_y, nz, slots), F32),
            pltpu.VMEM((own, slots), F32),
        ),
        in_specs=[VMEM, VMEM, VMEM, SMEM, SMEM],
        out_specs=(VMEM, VMEM),
        scratch_shapes=[
            pltpu.VMEM((4, total * 8, slots), F32),
            pltpu.VMEM((4, 3 * own * 8, slots), F32),
            pltpu.VMEM((total, 32, slots), BF16),
            pltpu.VMEM((3 * own, slots, 32), BF16),
            pltpu.VMEM((slots, 128), F32),
        ],
        compiler_params=PARAMS,
        cost_estimate=pl.CostEstimate(
            flops=own * 27 * slots * slots * 40, bytes_accessed=total * slots * 16, transcendentals=0
        ),
        name="density",
    )


def make_force(cells_y, nz, slots):
    sy = cells_y + 2
    own = cells_y * nz
    total = 3 * sy * nz
    chunk = 8

    def kernel(
        low, mid, high, slope_low, slope_mid, slope_high, electrons, repel, out,
        feature, extra, own_feature, own_extra, place, right, right_extra, left, left_extra, acc, sums,
    ):
        clear_spare(feature)
        clear_spare(own_feature)
        blocks = zip((low, mid, high), (slope_low, slope_mid, slope_high))
        for x, (block, slopes) in enumerate(blocks):
            for y in range(sy):
                pos = row_positions(block, x, y, sy, nz)
                square = pos[0] * pos[0] + pos[1] * pos[1] + pos[2] * pos[2]
                kind = channel(block, y, nz, 3)
                scale = by_kind(kind, repel)
                inverse = 1.0 / by_kind(kind, repel, 1.0)
                inverse = inverse * inverse
                steep = slopes[pl.ds(y * nz, nz), :] * inverse
                mild = -3.0 * by_kind(kind, electrons) * inverse
                double = 2.0 * scale
                values = [scale * (1.0 - square)] + [double * pos[d] for d in range(3)] + [-scale]
                cell = (x * sy + y) * nz
                store_five(feature, cell, nz, values, RIGHT)
                for d in range(3):
                    place[pl.ds(cell * 8 + d, nz, stride=8), :] = pos[d]
                for k in range(8):
                    extra[pl.ds(cell * 8 + k, nz, stride=8), :] = mild if k % 2 else steep
                if x == 1 and 1 <= y <= cells_y:
                    cell = (y - 1) * nz
                    for k in range(8):
                        own_extra[pl.ds(cell * 8 + k, nz, stride=8), :] = steep if k % 2 else mild
                    for dz in range(3):
                        across = pos[2] - (dz - 1.0)
                        square = pos[0] * pos[0] + pos[1] * pos[1] + across * across
                        values = [scale] + [
                            scale * value for value in (pos[0], pos[1], across, square)
                        ]
                        store_five(own_feature, dz * own + cell, nz, values, LEFT)

        fill(feature, own_feature, right, left)

        def fill_right_extra(n, carry):
            right_extra[n] = two_rows(extra[pl.ds(n * 8, 8), :], 0).astype(BF16)
            return carry

        def fill_left_extra(n, carry):
            left_extra[n] = two_rows(own_extra[pl.ds(n * 8, 8), :], 1).astype(BF16).T
            return carry

        lax.fori_loop(0, total, fill_right_extra, 0, unroll=8)
        lax.fori_loop(0, own, fill_left_extra, 0, unroll=8)
        same = same_slot(slots)
        lane = lax.broadcasted_iota(jnp.int32, (slots, 128), 1)
        sums[...] = jnp.zeros(sums.shape, F32)

        def one_cell(n, carry):
            y, z = n // nz, n % nz
            lhs_extra = left_extra[n]
            first = True
            for dz in range(3):
                zz = (z + (dz - 1 + nz)) % nz
                lhs = left[dz * own + n]
                near = [(dx * sy + y + dy) * nz + zz for dx in range(3) for dy in range(3)]
                if dz == 1:
                    near.append(near.pop(4))
                for index in range(0, 9, 2):
                    pair = near[index : index + 2]
                    rhs = [right[cell] for cell in pair]
                    rhs_extra = [right_extra[cell] for cell in pair]
                    if len(pair) > 1:
                        rhs = [jnp.concatenate(rhs, axis=1)]
                        rhs_extra = [jnp.concatenate(rhs_extra, axis=1)]
                    bare = dot(lhs, rhs[0], NN)
                    value = bare * dot(lhs_extra, rhs_extra[0], NN) - 2.0
                    weight = jnp.maximum(bare, 0.0)
                    if dz == 1 and index == 8:
                        weight = jnp.where(same, 0.0, weight)
                    value = value * weight
                    there = [
                        [place[pl.ds(cell * 8 + d, 1), :] for d in range(3)] for cell in pair
                    ]
                    if dz != 1:
                        there = [[x, y_, z_ + (dz - 1.0)] for x, y_, z_ in there]
                    for start in range(0, slots, chunk):
                        rows = pl.ds(start, chunk)
                        tiles = [
                            value[start : start + chunk, k * slots : (k + 1) * slots]
                            for k in range(len(pair))
                        ]
                        sums_of = [
                            [tile * there[k][d] for k, tile in enumerate(tiles)] for d in range(3)
                        ] + [tiles]
                        for d in range(4):
                            part = sums_of[d][0]
                            for more in sums_of[d][1:]:
                                part = part + more
                            acc[d, rows, :] = part if first else acc[d, rows, :] + part
                    first = False
            for d in range(4):
                column = jnp.sum(acc[d], axis=1, keepdims=True)
                sums[d] = jnp.where(lane == n, column, sums[d])
            return carry

        lax.fori_loop(0, own, one_cell, 0, unroll=8)
        rows = [sums[d].T for d in range(4)]
        for y in range(cells_y):
            pos = row_positions(mid, 1, y + 1, sy, nz)
            part = slice(y * nz, (y + 1) * nz)
            for d in range(3):
                out[d, y] = 2.0 * (rows[d][part] - pos[d] * rows[3][part])

    return pl.pallas_call(
        kernel,
        out_shape=pltpu.VMEM((3, cells_y, nz, slots), F32),
        in_specs=[VMEM] * 6 + [SMEM, SMEM],
        out_specs=VMEM,
        scratch_shapes=[
            pltpu.VMEM((4, total * 8, slots), F32),
            pltpu.VMEM((total * 8, slots), F32),
            pltpu.VMEM((4, 3 * own * 8, slots), F32),
            pltpu.VMEM((own * 8, slots), F32),
            pltpu.VMEM((total * 8, slots), F32),
            pltpu.VMEM((total, 32, slots), BF16),
            pltpu.VMEM((total, 16, slots), BF16),
            pltpu.VMEM((3 * own, slots, 32), BF16),
            pltpu.VMEM((own, slots, 16), BF16),
            pltpu.VMEM((4, slots, slots), F32),
            pltpu.VMEM((4, slots, 128), F32),
        ],
        compiler_params=PARAMS,
        cost_estimate=pl.CostEstimate(
            flops=own * 27 * slots * slots * 100,
            bytes_accessed=total * slots * 16,
            transcendentals=0,
        ),
        name="force",
    )


def shifted(axis, count):
    up = [(i, (i + 1) % count) for i in range(count)]
    down = [(target, source) for source, target in up]
    return lambda part: lax.ppermute(part, axis, up), lambda part: lax.ppermute(part, axis, down)


def halo(block, rows, gx, gy, gz):
    up, down = shifted("gy", gy)
    if gy == 2 and block.shape[0] == 2 * rows:
        other = up(block)
        low, high = other[-rows:], other[:rows]
    else:
        low, high = up(block[-rows:]), down(block[:rows])
    middle = jnp.concatenate([low, block, high], axis=0)
    up, down = shifted(("gx", "gz"), gx * gz)
    low = up(middle)
    high = down(middle)
    return low, middle, high


def on_device(
    cell_counts,
    grid_offset,
    fraction,
    species,
    species_density,
    species_pair,
    species_embed,
    species_charge,
):
    cells_x, cells_y, cells_z, _, slots = fraction.shape
    gx, gy, gz = (lax.axis_size(name) for name in ("gx", "gy", "gz"))
    devices = gx * gy * gz
    assert cells_x == gz and slots == 128
    lx, ly, lz = cells_x * gx * PPC, cells_y * gy * PPC, cells_z * gz * PPC
    assert lz % devices == 0
    modes = lz // devices
    yl = cells_y * PPC
    relayout = modes <= 128 and yl % max(1, 128 // modes) == 0

    slot_index = lax.broadcasted_iota(jnp.int32, species.shape, 3)
    alive = slot_index < cell_counts[..., None]
    kind = jnp.where(alive, species.astype(F32), -1.0)[:, :, None]

    atoms = jnp.concatenate(
        [
            grid_offset.astype(F32).transpose(0, 1, 3, 2, 4),
            fraction.transpose(0, 1, 3, 2, 4),
            kind,
        ],
        axis=2,
    )
    atoms = lax.all_to_all(atoms, "gz", split_axis=0, concat_axis=0, tiled=True)
    basis_x, basis_z = real_basis(lx), real_basis(lz)
    x_pair, xt_pair, z_pair = table_pair(basis_x), table_pair(basis_x.T), table_pair(basis_z)
    y_pair = table_pair(np.kron(real_basis(ly), np.eye(modes)))
    spread = make_spread(gz, cells_y, cells_z, slots, lz, devices, relayout)
    lines = spread(near_core(atoms), species_charge, z_pair)
    if not relayout:
        lines = lines.reshape(yl, PPC, devices, modes).transpose(2, 1, 0, 3)
        lines = lines.reshape(devices, PPC, yl * modes)
    planes = lax.all_to_all(lines, ("gx", "gy", "gz"), split_axis=0, concat_axis=0, tiled=True)

    nz = gz * cells_z
    place = (atoms[:, :, 0:3] + 0.5 + atoms[:, :, 3:6]) / PPC - 0.5
    place = jnp.concatenate([place, atoms[:, :, 6:7]], axis=2)
    place = place.transpose(1, 2, 0, 3, 4).reshape(cells_y * 4 * nz, slots)
    near = halo(place, nz * 4, gx, gy, gz)
    density, slope = make_density(cells_y, nz, slots)(
        *map(near_core, near), species_density, species_embed
    )
    near_slopes = halo(slope, nz, gx, gy, gz)

    rank = lax.axis_index(("gx", "gy", "gz")).astype(jnp.int32).reshape(1)
    planes = make_planes(gx, gy, gz, yl * modes, lx, ly, lz)(
        rank, near_core(planes), x_pair.reshape(2 * lx, lx), xt_pair.reshape(2 * lx, lx), near_core(y_pair)
    )
    lines = lax.all_to_all(planes, ("gx", "gy", "gz"), split_axis=0, concat_axis=0, tiled=True)
    if not relayout:
        lines = lines.reshape(devices, PPC, yl, modes).transpose(2, 1, 0, 3)
        lines = lines.reshape(yl * PPC, lz)

    operands = (*near, *near_slopes)
    short = make_force(cells_y, nz, slots)(*map(near_core, operands), species_density, species_pair)
    result = make_sample(gz, cells_y, cells_z, slots, lz, devices, relayout)(
        near_core(lines), near_core(atoms), near_core(short), near_core(density), species_charge, z_pair
    )
    result = lax.all_to_all(result, "gz", split_axis=0, concat_axis=0, tiled=True)
    forces, density = make_finish(result.shape)(near_core(result))
    return (forces.transpose(0, 1, 3, 2, 4), density)


def solution(mesh):
    return jax.shard_map(
        on_device,
        mesh=mesh,
        in_specs=(
            P("gx", "gy", "gz"),
            P("gx", "gy", "gz", None, None),
            P("gx", "gy", "gz", None, None),
            P("gx", "gy", "gz", None),
            P(),
            P(),
            P(),
            P(),
        ),
        out_specs=(P("gx", "gy", "gz", None, None), P("gx", "gy", "gz", None)),
        check_vma=False,
    )
```
